128 devices in a mesh: row: 16 (over x, y), col: 8 (over z, core).
Axes of the slice: x: 4, y: 4, z: 4, core: 2. Of those that a mesh axis runs over, the one named last changes fastest.
Arguments:
- design: bfloat16 [16384, 6144], P(('row', 'col')), may hold values from -0.046875 to 0.046875
- observations: float32 [16384], P(('row', 'col')), may hold values from -6 to 6
- gaps: int32 [16384], P(('row', 'col')), may hold values 0 or 1
- noise_var: float32 [16384], P(('row', 'col')), may hold values from 0.25 to 4
- arc_lengths: int32 [128, 4], P(('row', 'col')), may hold values from 1 to 64, 128 in all within a row
- arc_amp: float32 [128, 4], P(('row', 'col')), may hold values from 0.2 to 2
- arc_decay: float32 [128, 4], P(('row', 'col')), may hold values from 0.3 to 0.95
- plan: int32 [128], P(('row', 'col')), may hold values from 0 to 127, each once
- tile_map: int32 [48], replicated, may hold values from 0 to 47, each once
Outputs:
- gram: float32 [6144, 6144], P('row', 'col')
- normal_rhs: float32 [6144], P('row')
- balanced_obs: float32 [128, 128], P(('row', 'col'))
The draws below stay inside these ranges and needn't reach their ends.
Inputs may be any that keep to these rules, and one draw needn't show every extreme that they name: `plan`: a permutation of the blocks. `tile_map`: a permutation of the tiles. `arc_lengths`: each block's arc lengths sum to 128; some arc has 64 rows.
All inputs are finite; a program needn't handle non-finite values. No bound on the sum of `gaps` on one device may be relied on, other than what follows from the above.
Results may differ from the reference program's by a relative error of at most 0.004.
Values may be sent and summed in bfloat16 or wider, within the bound.
A program may use at most 192 MiB of HBM per device.

```python
import math
import jax
import jax.numpy as jnp
import numpy as np
from jax import lax

U = 6144
TB = 128
SB = 128
ARCS = 4
MAXARC = 64
BLOCKS = 128
ROWS = 16384


def set_ends(values, rng, low, high):
    longest = values.shape.index(max(values.shape))
    spots = []
    for shift in (0, 1):
        where = [jax.random.randint(jax.random.fold_in(rng, axis), (), 0, length) for axis, length in enumerate(values.shape)]
        where[longest] = (where[longest] + shift) % values.shape[longest]
        spots.append(tuple(where))
    return values.at[spots[0]].set(low).at[spots[1]].set(high)


def level_of(rng, shape, cuts, smallest, high):
    factor_of, own = 1.0, jax.random.fold_in(rng, 6)
    for dim, blocks in cuts:
        draws = jnp.exp(jax.random.uniform(jax.random.fold_in(own, dim), (blocks,), jnp.float32, smallest / len(cuts), high / len(cuts)))
        factor_of = factor_of * jnp.repeat(draws, shape[dim] // blocks).reshape([-1 if axis == dim else 1 for axis in range(len(shape))])
    return factor_of


def profile(count, total, reach, slope):
    weights = [(1 << 20) // math.isqrt(grade ** slope) + 1 for grade in range(2, count + 1)]
    rest, given = total - reach - (count - 1), [1] * (count - 1)
    while rest > 0:
        candidates = [i for i in range(count - 1) if given[i] < reach]
        mass, budget = sum([weights[i] for i in candidates]), rest
        for i in candidates:
            extra = min(reach - given[i], max(1, budget * weights[i] // mass), rest)
            given[i] = given[i] + extra
            rest = rest - extra
    return np.array([reach] + given)


def uneven_parts(own_key, count, total, bound, skew):
    if count == 2:
        one = jax.random.randint(own_key, (), max(1, total - bound), min(bound, total - 1) + 1)
        return jnp.stack([one, total - one])
    sizes = jnp.asarray(profile(count, total, bound, skew), jnp.int32)
    pairs = (count - 1) // 2
    giver, receiver = sizes[1:1 + 2 * pairs:2], sizes[2:2 + 2 * pairs:2]
    room = jnp.minimum(giver - 1, bound - receiver)
    shifted = jax.random.randint(jax.random.fold_in(own_key, 1), (pairs,), 0, 1 << 20) % (room + 1)
    sizes = sizes.at[1:1 + 2 * pairs:2].set(giver - shifted).at[2:2 + 2 * pairs:2].set(receiver + shifted)
    return sizes[jax.random.permutation(jax.random.fold_in(own_key, 2), count)]


def gaussian(key, dims, deviation, most, split=(), held_as=jnp.bfloat16):
    array = jax.random.normal(key, dims, jnp.float32) * deviation
    if len(split) > 0:
        array = level_of(key, dims, split, -0.22, 0.18) * array
    return jnp.clip(array, min=-most, max=most).astype(held_as)


def setup_inputs(seed: int = 0) -> dict:
    key_list = jax.random.split(jax.random.key(seed), 10)
    return {
        "design": gaussian(key_list[0], (ROWS, U), (ROWS ** -0.5), 0.046875, ((0, 128),)),
        "observations": gaussian(key_list[1], (ROWS,), 1.0, 6.0, ((0, 128),), jnp.float32),
        "gaps": set_ends((jax.random.randint(key_list[2], (ROWS,), 0, 8) < 7).astype(jnp.int32), jax.random.fold_in(key_list[2], 1), 0, 1),
        "noise_var": jnp.clip(jnp.exp(math.log(4.0) - 2.7725887 * jax.random.uniform(key_list[3], (ROWS,), jnp.float32) ** level_of(key_list[3], (ROWS,), ((0, 128),), -0.2, 0.2)), 0.25, 4.0),
        "arc_lengths": jax.vmap(lambda own: uneven_parts(own, ARCS, SB, MAXARC, 2))(jax.random.split(key_list[4], BLOCKS)).reshape((BLOCKS, ARCS)).astype(jnp.int32),
        "arc_amp": jnp.clip(jnp.exp(math.log(2.0) - 2.3025851 * jax.random.uniform(key_list[5], (BLOCKS, ARCS), jnp.float32) ** level_of(key_list[5], (BLOCKS, ARCS), ((0, 128),), -0.2, 0.2)), 0.2, 2.0),
        "arc_decay": jnp.clip(0.3 + 0.65 * jax.random.uniform(key_list[6], (BLOCKS, ARCS), jnp.float32) ** level_of(key_list[6], (BLOCKS, ARCS), ((0, 128),), -0.2, 0.2), 0.3, 0.95),
        "plan": jax.random.permutation(key_list[7], BLOCKS).astype(jnp.int32),
        "tile_map": jax.random.permutation(key_list[8], U // TB).astype(jnp.int32),
    }


def whiten(block, obs_rows, live_rows, noise_rows, lengths, amplitude, decay):
    block_rows = block.shape[0]
    arc_count = lengths.shape[0]
    position = jnp.arange(block_rows, dtype=jnp.int32)
    arc_ends = jnp.cumsum(lengths).astype(jnp.int32)
    arc_id = jnp.sum((arc_ends[None, :] <= position[:, None]).astype(jnp.int32), axis=1)
    member = (arc_id[:, None] == jnp.arange(arc_count, dtype=jnp.int32)[None, :]).astype(jnp.float32)
    row_amp = jnp.sum(member * amplitude[None, :], axis=1)
    row_rate = jnp.sum(member * jnp.log(decay)[None, :], axis=1)
    same_arc = (arc_id[:, None] == arc_id[None, :]).astype(jnp.float32)
    row_lag = jnp.abs(position[:, None] - position[None, :]).astype(jnp.float32)
    kernel = row_amp[:, None] * jnp.exp(row_lag * row_rate[:, None]) * same_arc * live_rows[:, None] * live_rows[None, :]
    covariance = kernel + jnp.diag(noise_rows)
    factor = jnp.linalg.cholesky(covariance)
    solved = lax.linalg.triangular_solve(factor, block.astype(jnp.float32) * live_rows[:, None], left_side=True, lower=True)
    solved_obs = lax.linalg.triangular_solve(factor, (obs_rows * live_rows)[:, None], left_side=True, lower=True)
    return (solved.astype(jnp.bfloat16), solved_obs[:, 0])

def reference(design, observations, gaps, noise_var, arc_lengths, arc_amp, arc_decay, plan, tile_map):
    block_count = arc_lengths.shape[0]
    block_rows = design.shape[0] // block_count
    columns = design.shape[1]
    tile_count = tile_map.shape[0]
    tile_size = columns // tile_count
    live_rows = gaps.astype(jnp.float32)

    def one_block(inputs):
        return whiten(*inputs)
    white, white_obs = lax.map(one_block, (design.reshape(block_count, block_rows, columns), observations.reshape(block_count, block_rows), live_rows.reshape(block_count, block_rows), noise_var.reshape(block_count, block_rows), arc_lengths, arc_amp, arc_decay))
    slotted = white.reshape(-1, tile_count, tile_size)[:, tile_map, :].reshape(-1, columns)
    widened = slotted.astype(jnp.float32)
    gram = jnp.dot(widened.T, widened, precision=lax.Precision.HIGHEST)
    obs_half = white_obs.reshape(-1).astype(jnp.bfloat16)
    normal_rhs = jnp.dot(obs_half.astype(jnp.float32), slotted.astype(jnp.float32), preferred_element_type=jnp.float32)
    balanced_obs = white_obs[plan]
    return (gram, normal_rhs, balanced_obs)
```

```python
import jax
import jax.numpy as jnp
from jax import lax
from jax.experimental import pallas as pl
from jax.experimental.pallas import tpu as pltpu
from jax.sharding import PartitionSpec as P

MESH = pl.DeviceIdType.MESH
F32 = jnp.float32
BF16 = jnp.bfloat16
TB = 128
R_DX = (2, 1, 3, 0)
C_CH = ((0, 2), (2, 2), (4, 2))
NA, NB = len(R_DX), len(C_CH)
N_COPIES = 126


def inverse_factor(lens, amps, decays, gaps, noise, obs):
    shape = (8, TB)
    pos = lax.broadcasted_iota(jnp.int32, shape, 1)
    live = jnp.broadcast_to(gaps, shape).astype(F32)
    noise = jnp.broadcast_to(noise, shape)
    e0 = lens[0, 0]
    e1 = e0 + lens[0, 1]
    e2 = e1 + lens[0, 2]

    def by_arc(p, v):
        return jnp.where(p < e0, v[0], jnp.where(p < e1, v[1], jnp.where(p < e2, v[2], v[3])))

    amp = by_arc(pos, [amps[0, i] for i in range(4)])
    decay = by_arc(pos, [decays[0, i] for i in range(4)])
    start = (pos == 0) | (pos == e0) | (pos == e1) | (pos == e2)
    gain = decay * decay
    q = amp * (1.0 - gain)
    live_prev = pltpu.roll(live, 1, 1) > 0.5
    noise_prev = pltpu.roll(noise, 1, 1)
    a = jnp.where(start, 0.0, jnp.where(live_prev, gain * noise_prev + q, gain))
    b = jnp.where(start, amp, jnp.where(live_prev, q * noise_prev, q))
    c = jnp.where(start, 0.0, jnp.where(live_prev, 1.0, 0.0))
    d = jnp.where(start, 1.0, jnp.where(live_prev, noise_prev, 1.0))
    for shift in (1, 2, 4, 8, 16, 32):
        ok = pos >= shift
        ap, bp = pltpu.roll(a, shift, 1), pltpu.roll(b, shift, 1)
        cp, dp = pltpu.roll(c, shift, 1), pltpu.roll(d, shift, 1)
        an = jnp.where(ok, a * ap + b * cp, a)
        bn = jnp.where(ok, a * bp + b * dp, b)
        cn = jnp.where(ok, c * ap + d * cp, c)
        dn = jnp.where(ok, c * bp + d * dp, d)
        scale = 1.0 / (an + bn + cn + dn)
        a, b, c, d = an * scale, bn * scale, cn * scale, dn * scale
    var = b / d
    is_live = live > 0.5
    total = jnp.where(is_live, var, 0.0) + noise
    root = live * lax.rsqrt(total)
    log_step = jnp.log(jnp.where(is_live, decay * (noise / total), decay))
    push = jnp.where(is_live, decay * (var / total), 0.0)
    sq = (TB, TB)
    row = lax.broadcasted_iota(jnp.int32, sq, 0)
    col = lax.broadcasted_iota(jnp.int32, sq, 1)
    upto = (row <= col).astype(F32)
    cum = jnp.dot(log_step, upto, precision=lax.Precision.HIGHEST, preferred_element_type=F32)
    before = cum - log_step
    eye = row == col

    def as_column(v):
        return jnp.sum(jnp.where(eye, jnp.broadcast_to(v[0:1], sq), 0.0), axis=1, keepdims=True)

    def arc_of(p):
        return by_arc(p, [0, 1, 2, 3])

    inside = (row > col) & (arc_of(row) == arc_of(col))
    span = jnp.where(inside, as_column(before) - cum[0:1], -1e30)
    lower = jnp.where(eye, 1.0, -jnp.exp(span) * push[0:1])
    inv = as_column(root) * lower
    white_col = jnp.sum(inv * obs, axis=1, keepdims=True)
    white_row = jnp.sum(jnp.where(eye, white_col, 0.0), axis=0, keepdims=True)
    return inv, white_row


def kernel(
    tile_map, lens, amps, decays, plan, design, obs, gaps, noise,
    gram, rhs, bal,
    dbuf, wn, wt, pall, rbuf, rsend, cbufs, csends, acc, rss, rsr, obs_all, psend, pbuf, qbuf, tot, tbuf,
    load_sem, ssem, rsem,
):
    r, q = lax.axis_index("row"), lax.axis_index("col")
    x, y, z, c = r // 4, r % 4, q // 2, q % 2

    def dev(dx=0, dy=0, dz=0, dc=0):
        return ((x + dx) % 4 * 4 + (y + dy) % 4, (z + dz) % 4 * 2 + (c + dc) % 2)

    copies = []

    def send(src, dst, to):
        i = len(copies)
        cp = pltpu.make_async_remote_copy(
            src_ref=src, dst_ref=dst, send_sem=ssem.at[i], recv_sem=rsem.at[i], device_id=to, device_id_type=MESH
        )
        cp.start()
        copies.append(cp)
        return cp

    load = pltpu.make_async_copy(design, dbuf, load_sem)
    load.start()
    line = [(dz, dc) for dz in range(4) for dc in range(2) if (dz, dc) != (0, 0)]
    partners = [dev(dx=i) for i in (1, 2, 3)] + [dev(dy=i) for i in (1, 2, 3)] + [dev(dz=i, dc=j) for i, j in line]
    barrier = pltpu.get_barrier_semaphore()
    for p in partners:
        pl.semaphore_signal(barrier, inc=1, device_id=p, device_id_type=MESH)

    inv, white_row = inverse_factor(lens, amps, decays, gaps[...], noise[...], obs[...])
    hi = inv.astype(BF16)
    lo = (inv - hi.astype(F32)).astype(BF16)
    both = jnp.concatenate([hi, lo], axis=1)
    obs_all[r, q] = white_row
    half = jnp.broadcast_to(white_row, (8, TB)).astype(BF16)
    load.wait()

    def whiten_pair(t, carry):
        cols = dbuf[:, pl.ds(pl.multiple_of(t * 256, 256), 256)]
        white = jnp.dot(both, jnp.concatenate([cols, cols], axis=0), preferred_element_type=F32)
        kept = white.astype(BF16)
        flipped = white.T.astype(BF16)
        part = jnp.dot(half, kept, preferred_element_type=F32)
        for i in range(2):
            wn[2 * t + i] = kept[:, i * TB : (i + 1) * TB]
            wt[2 * t + i] = flipped[i * TB : (i + 1) * TB]
            pall[2 * t + i] = part[0:1, i * TB : (i + 1) * TB]
        return carry

    lax.fori_loop(0, 24, whiten_pair, 0, unroll=2)

    for k, dx in enumerate(R_DX):
        for dy in range(4):
            for i in range(3):
                t = tile_map[(x + dx) % 4 * 12 + (y + dy) % 4 * 3 + i]
                rows = pl.ds(i * TB, TB)
                if dy == 0:
                    rbuf[k, 0, 0, 0, rows] = wt[t]
                else:
                    rsend[k, dy - 1, rows] = wt[t]
    for b, (first, count) in enumerate(C_CH):
        for dz in range(4):
            for dc in range(2):
                for i in range(count):
                    t = tile_map[((z + dz) % 4 * 2 + (c + dc) % 2) * 6 + first + i]
                    cols = pl.ds(i * TB, TB)
                    if (dz, dc) == (0, 0):
                        cbufs[b][0, 0, :, cols] = wn[t]
                    else:
                        csends[b][dz * 2 + dc - 1, :, cols] = wn[t]
    for dy in range(4):
        for xx in range(4):
            for i in range(3):
                t = tile_map[xx * 12 + (y + dy) % 4 * 3 + i]
                psend[dy, xx, i : i + 1] = pall[t]

    pl.semaphore_wait(barrier, len(partners))

    partner = dev(dc=1)
    y_up, y_dn, z_up, z_dn = dev(dy=1), dev(dy=3), dev(dz=1), dev(dz=3)

    def spread_r(k):
        return [send(rsend.at[k, d - 1], rbuf.at[k, 0, 0, 4 - d], dev(dy=d)) for d in (1, 3, 2)]

    def spread_c(b):
        return [
            send(csends[b].at[dz * 2 + dc - 1], cbufs[b].at[0, (4 - dz) % 4 * 2 + dc], dev(dz=dz, dc=dc))
            for dz, dc in line
        ]

    def gather1(buf, up, dn, halves):
        first, second = halves
        return [
            send(buf(0, first), buf(3, first), up),
            send(buf(0, second), buf(1, second), dn),
            send(buf(0, second), buf(3, second), up),
            send(buf(0, first), buf(1, first), dn),
        ]

    def gather2(buf, up, dn, halves, sent):
        first, second = halves
        sent[0].wait_recv()
        a = send(buf(3, first), buf(2, first), up)
        sent[1].wait_recv()
        return [a, send(buf(1, second), buf(2, second), dn)]

    r_halves = (pl.ds(0, 2), pl.ds(2, 2))
    c_halves = (pl.ds(0, 4), pl.ds(4, 4))
    r_ref = [lambda rz, part, k=k: rbuf.at[k, rz, 0, part] for k in range(NA)]
    c_ref = [lambda ry, part, b=b: cbufs[b].at[ry, part] for b in range(NB)]
    a2a_r, a2a_c, g1r, g2r, g1c, g2c = {}, {}, {}, {}, {}, {}
    d2d = {k: [] for k in range(NA)}

    def over(k, rz):
        d2d[k].append(send(rbuf.at[k, rz, 0], rbuf.at[k, rz, 1], partner))

    def r1(k):
        for cp in a2a_r[k]:
            cp.wait_recv()
        g1r[k] = gather1(r_ref[k], z_up, z_dn, r_halves)
        over(k, 0)

    def r2(k):
        g2r[k] = gather2(r_ref[k], z_up, z_dn, r_halves, g1r[k])

    def rd(k):
        g1r[k][2].wait_recv()
        over(k, 3)
        g1r[k][3].wait_recv()
        over(k, 1)

    def re(k):
        for cp in g2r[k]:
            cp.wait_recv()
        over(k, 2)

    def rf(k):
        for cp in d2d[k]:
            cp.wait_recv()

    def c1(b):
        for cp in a2a_c[b]:
            cp.wait_recv()
        g1c[b] = gather1(c_ref[b], y_up, y_dn, c_halves)

    def c2(b):
        g2c[b] = gather2(c_ref[b], y_up, y_dn, c_halves, g1c[b])

    def cf(b):
        for cp in g1c[b][2:] + g2c[b]:
            cp.wait_recv()

    reduce = {}

    def block(k, b):
        first, count = C_CH[b]
        out = gram.at[:, pl.ds(first * TB, count * TB)] if R_DX[k] == 0 else acc.at[:, pl.ds(0, count * TB)]

        def product(rz):
            lhs = jnp.concatenate([rbuf[k, rz, rc, ry] for rc in range(2) for ry in range(4)], axis=1)
            right = jnp.concatenate([cbufs[b][ry, rz * 2 + rc] for rc in range(2) for ry in range(4)], axis=0)
            return jnp.dot(lhs, right, preferred_element_type=F32)

        out[...] = product(0)

        def step(rz, carry):
            out[...] += product(rz)
            return carry

        lax.fori_loop(1, 4, step, 0)
        dx = R_DX[k]
        if dx:
            rss[b][dx - 1] = out[...].astype(BF16)
            reduce[b, dx] = send(rss[b].at[dx - 1], rsr[b].at[3 - dx], dev(dx=dx))

    def small1():
        o = [send(obs_all.at[r, q], obs_all.at[r, q], dev(dz=dz, dc=dc)) for dz, dc in line]
        pbuf[y] = psend[0]
        p = [send(psend.at[d], pbuf.at[y], dev(dy=d)) for d in (1, 2, 3)]
        return o + p

    def small2(sent):
        for cp in sent:
            cp.wait_recv()
        o = [send(obs_all.at[r], obs_all.at[r], dev(dy=d)) for d in (1, 2, 3)]
        qbuf[q] = (pbuf[0] + pbuf[1]) + (pbuf[2] + pbuf[3])
        p = [send(qbuf.at[q], qbuf.at[q], dev(dz=dz, dc=dc)) for dz, dc in line]
        return o + p

    def small3(sent):
        for cp in sent:
            cp.wait_recv()
        rows = obs_all.at[pl.ds(4 * x, 4)]
        o = [send(rows, rows, dev(dx=d)) for d in (1, 2, 3)]
        total = qbuf[0]
        for i in range(1, 8):
            total = total + qbuf[i]
        tot[...] = total
        tbuf[x] = tot[x]
        p = [send(tot.at[(x + d) % 4], tbuf.at[x], dev(dx=d)) for d in (1, 2, 3)]
        return o + p

    def small4(sent):
        for cp in sent:
            cp.wait_recv()
        rhs[...] = (tbuf[0] + tbuf[1]) + (tbuf[2] + tbuf[3])
        owner = plan[0]
        bal[...] = obs_all[owner // 8, owner % 8]

    a2a_r[0] = spread_r(0)
    a2a_c[0] = spread_c(0)
    a2a_r[1] = spread_r(1)
    small = small1()
    r1(0)
    c1(0)
    a2a_c[1] = spread_c(1)
    a2a_r[2] = spread_r(2)
    r2(0)
    r1(1)
    c2(0)
    c1(1)
    rd(0)
    a2a_c[2] = spread_c(2)
    a2a_r[3] = spread_r(3)
    re(0)
    rf(0)
    cf(0)
    block(0, 0)
    r2(1)
    r1(2)
    c2(1)
    c1(2)
    rd(1)
    re(1)
    small = small2(small)
    rf(1)
    block(1, 0)
    cf(1)
    block(0, 1)
    block(1, 1)
    r2(2)
    r1(3)
    rd(2)
    c2(2)
    re(2)
    small = small3(small)
    rf(2)
    block(2, 0)
    block(2, 1)
    r2(3)
    rd(3)
    re(3)
    cf(2)
    block(0, 2)
    block(1, 2)
    block(2, 2)
    rf(3)
    for b in range(NB):
        block(3, b)
    small4(small)
    for b, (first, count) in enumerate(C_CH):
        total = gram[:, first * TB : (first + count) * TB]
        for dx in (1, 3, 2):
            reduce[b, dx].wait_recv()
        for i in range(3):
            total = total + rsr[b][i].astype(F32)
        gram[:, first * TB : (first + count) * TB] = total
    for cp in copies:
        cp.wait_send()


def on_device(
    design, observations, gaps, noise_var, arc_lengths, arc_amp, arc_decay, plan, tile_map
):
    smem = pl.BlockSpec(memory_space=pltpu.SMEM)
    vmem = pl.BlockSpec(memory_space=pltpu.VMEM)
    width = [count * TB for _, count in C_CH]
    gram, rhs, bal = pl.pallas_call(
        kernel,
        name="normal_equations",
        out_shape=(
            jax.ShapeDtypeStruct((384, 768), F32),
            jax.ShapeDtypeStruct((3, TB), F32),
            jax.ShapeDtypeStruct((1, TB), F32),
        ),
        in_specs=[smem] * 5 + [pl.BlockSpec(memory_space=pl.ANY)] + [vmem] * 3,
        out_specs=(vmem, vmem, vmem),
        scratch_shapes=[
            pltpu.VMEM((TB, 6144), BF16),
            pltpu.VMEM((48, TB, TB), BF16),
            pltpu.VMEM((48, TB, TB), BF16),
            pltpu.VMEM((48, 1, TB), F32),
            pltpu.VMEM((NA, 4, 2, 4, 384, TB), BF16),
            pltpu.VMEM((NA, 3, 384, TB), BF16),
            [pltpu.VMEM((4, 8, TB, w), BF16) for w in width],
            [pltpu.VMEM((7, TB, w), BF16) for w in width],
            pltpu.VMEM((384, max(width)), F32),
            [pltpu.VMEM((3, 384, w), BF16) for w in width],
            [pltpu.VMEM((3, 384, w), BF16) for w in width],
            pltpu.VMEM((16, 8, 1, TB), F32),
            pltpu.VMEM((4, 4, 3, TB), F32),
            pltpu.VMEM((4, 4, 3, TB), F32),
            pltpu.VMEM((8, 4, 3, TB), F32),
            pltpu.VMEM((4, 3, TB), F32),
            pltpu.VMEM((4, 3, TB), F32),
            pltpu.SemaphoreType.DMA,
            pltpu.SemaphoreType.DMA((N_COPIES,)),
            pltpu.SemaphoreType.DMA((N_COPIES,)),
        ],
        compiler_params=pltpu.CompilerParams(
            collective_id=0, has_side_effects=True, vmem_limit_bytes=60 * 1024 * 1024
        ),
    )(
        tile_map,
        arc_lengths,
        arc_amp,
        arc_decay,
        plan,
        design,
        observations.reshape(1, TB),
        gaps.reshape(1, TB),
        noise_var.reshape(1, TB),
    )
    return gram, rhs.reshape(384), bal


def solution(mesh):
    placed = (
        P(("row", "col"), None),
        P(("row", "col")),
        P(("row", "col")),
        P(("row", "col")),
        P(("row", "col"), None),
        P(("row", "col"), None),
        P(("row", "col"), None),
        P(("row", "col")),
        P(),
    )
    return jax.shard_map(
        on_device,
        mesh=mesh,
        in_specs=placed,
        out_specs=(P("row", "col"), P("row"), P(("row", "col"), None)),
        check_vma=False,
    )
```

```python
import jax
import jax.numpy as jnp
from jax import lax
from jax.experimental import pallas as pl
from jax.experimental.pallas import tpu as pltpu
from jax.sharding import PartitionSpec as P

MESH = pl.DeviceIdType.MESH
F32 = jnp.float32
BF16 = jnp.bfloat16
TB = 128
R_CH = (((2, 0, 384),), ((1, 0, 192), (3, 0, 192)), ((1, 192, 192), (3, 192, 192)), ((0, 0, 384),))
C_CH = ((0, 2), (2, 2), (4, 1), (5, 1))
NA, NB, NJ = len(R_CH), len(C_CH), 6
ORDER = (
    (0, 0, 1), (1, 0, 1), (0, 2, 3), (1, 2, 3), (2, 0, 1), (2, 2, 3), (0, 4, 4), (1, 4, 4), (2, 4, 4),
    (0, 5, 5), (1, 5, 5), (2, 5, 5), (3, 0, 1), (3, 2, 3), (3, 4, 5),
)
N_GOT, N_LEFT = 50, 13


def inverse_factor(lens, amps, decays, gaps, noise, obs):
    shape = (8, TB)
    pos = lax.broadcasted_iota(jnp.int32, shape, 1)
    live = jnp.broadcast_to(gaps, shape).astype(F32)
    noise = jnp.broadcast_to(noise, shape)
    e0 = lens[0, 0]
    e1 = e0 + lens[0, 1]
    e2 = e1 + lens[0, 2]

    def by_arc(p, v):
        return jnp.where(p < e0, v[0], jnp.where(p < e1, v[1], jnp.where(p < e2, v[2], v[3])))

    amp = by_arc(pos, [amps[0, i] for i in range(4)])
    decay = by_arc(pos, [decays[0, i] for i in range(4)])
    start = (pos == 0) | (pos == e0) | (pos == e1) | (pos == e2)
    gain = decay * decay
    q = amp * (1.0 - gain)
    live_prev = pltpu.roll(live, 1, 1) > 0.5
    noise_prev = pltpu.roll(noise, 1, 1)
    a = jnp.where(start, 0.0, jnp.where(live_prev, gain * noise_prev + q, gain))
    b = jnp.where(start, amp, jnp.where(live_prev, q * noise_prev, q))
    c = jnp.where(start, 0.0, jnp.where(live_prev, 1.0, 0.0))
    d = jnp.where(start, 1.0, jnp.where(live_prev, noise_prev, 1.0))
    for shift in (1, 2, 4, 8, 16, 32):
        ok = pos >= shift
        ap, bp = pltpu.roll(a, shift, 1), pltpu.roll(b, shift, 1)
        cp, dp = pltpu.roll(c, shift, 1), pltpu.roll(d, shift, 1)
        an = jnp.where(ok, a * ap + b * cp, a)
        bn = jnp.where(ok, a * bp + b * dp, b)
        cn = jnp.where(ok, c * ap + d * cp, c)
        dn = jnp.where(ok, c * bp + d * dp, d)
        scale = 1.0 / (an + bn + cn + dn)
        a, b, c, d = an * scale, bn * scale, cn * scale, dn * scale
    var = b / d
    is_live = live > 0.5
    total = jnp.where(is_live, var, 0.0) + noise
    root = live * lax.rsqrt(total)
    log_step = jnp.log(jnp.where(is_live, decay * (noise / total), decay))
    push = jnp.where(is_live, decay * (var / total), 0.0)
    sq = (TB, TB)
    row = lax.broadcasted_iota(jnp.int32, sq, 0)
    col = lax.broadcasted_iota(jnp.int32, sq, 1)
    upto = (row <= col).astype(F32)
    cum = jnp.dot(log_step, upto, precision=lax.Precision.HIGHEST, preferred_element_type=F32)
    before = cum - log_step
    eye = row == col

    def as_column(v):
        return jnp.sum(jnp.where(eye, jnp.broadcast_to(v[0:1], sq), 0.0), axis=1, keepdims=True)

    def arc_of(p):
        return by_arc(p, [0, 1, 2, 3])

    inside = (row > col) & (arc_of(row) == arc_of(col))
    span = jnp.where(inside, as_column(before) - cum[0:1], -1e30)
    lower = jnp.where(eye, 1.0, -jnp.exp(span) * push[0:1])
    inv = as_column(root) * lower
    white_col = jnp.sum(inv * obs, axis=1, keepdims=True)
    white_row = jnp.sum(jnp.where(eye, white_col, 0.0), axis=0, keepdims=True)
    return inv, white_row


def kernel(
    tile_map, lens, amps, decays, plan, design, obs, gaps, noise,
    gram, rhs, bal,
    vbuf, gbuf, dbuf, wn, wt, pall, rbuf, rsend, cbuf, csend, own, rss, rsr, obs_all, psend, pbuf, qbuf, tot, tbuf,
    load_sem, ssem, rsem, sum_ssem, sum_rsem,
):
    r, q = lax.axis_index("row"), lax.axis_index("col")
    x, y, z, c = r // 4, r % 4, q // 2, q % 2

    def place(dx, dy, dz, dc):
        return ((x + dx) % 4 * 4 + (y + dy) % 4, (z + dz) % 4 * 2 + (c + dc) % 2)

    steps = [(i, 0, 0, 0) for i in (1, 2, 3)] + [(0, i, 0, 0) for i in (1, 2, 3)]
    steps = steps + [(0, 0, i, j) for i in range(4) for j in range(2) if (i, j) != (0, 0)]
    places = {step: place(*step) for step in steps}

    def dev(dx=0, dy=0, dz=0, dc=0):
        return places[dx, dy, dz, dc]

    x_of = [(x + d) % 4 for d in range(4)]
    x_rows = pl.ds(4 * x, 4)

    got, left = {}, {}

    def group(table, sems, name, region):
        if name not in table:
            table[name] = (len(table), sems, region)
        return table[name][0]

    def wait(table, name):
        i, sems, region = table[name]
        pltpu.make_async_copy(region(), region(), sems.at[i]).wait()

    def send(src, dst, to, arrival, leaving):
        pltpu.make_async_remote_copy(
            src_ref=src, dst_ref=dst, send_sem=ssem.at[group(left, ssem, *leaving)], recv_sem=rsem.at[group(got, rsem, *arrival)],
            device_id=to, device_id_type=MESH,
        ).start()

    load = pltpu.make_async_copy(design, dbuf, load_sem.at[0])
    vectors = [
        pltpu.make_async_copy(ref, vbuf.at[i], load_sem.at[1 + i]) for i, ref in enumerate((obs, noise))
    ] + [pltpu.make_async_copy(gaps, gbuf, load_sem.at[3])]
    line = [(dz, dc) for dz in range(4) for dc in range(2) if (dz, dc) != (0, 0)]
    barrier = pltpu.get_barrier_semaphore()
    for p in places.values():
        pl.semaphore_signal(barrier, inc=1, device_id=p, device_id_type=MESH)

    for cp in vectors:
        cp.start()
    load.start()
    for cp in vectors:
        cp.wait()
    inv, white_row = inverse_factor(lens, amps, decays, gbuf[...], vbuf[1], vbuf[0])
    hi = inv.astype(BF16)
    lo = (inv - hi.astype(F32)).astype(BF16)
    both = jnp.concatenate([hi, lo], axis=1)
    obs_all[r, q] = white_row
    half = jnp.broadcast_to(white_row, (8, TB)).astype(BF16)
    load.wait()

    def whiten_pair(t, carry):
        cols = dbuf[:, pl.ds(pl.multiple_of(t * 256, 256), 256)]
        white = jnp.dot(both, jnp.concatenate([cols, cols], axis=0), preferred_element_type=F32)
        kept = white.astype(BF16)
        flipped = white.T.astype(BF16)
        for i in range(2):
            wn[2 * t + i] = kept[:, i * TB : (i + 1) * TB]
            wt[2 * t + i] = flipped[i * TB : (i + 1) * TB]
        return carry

    lax.fori_loop(0, 24, whiten_pair, 0, unroll=6)

    def stage_r(k):
        for dy in range(4):
            at = 0
            for dx, first, count in R_CH[k]:
                for i in range(3):
                    lo, hi = max(first, i * TB), min(first + count, i * TB + TB)
                    if lo < hi:
                        t = tile_map[(x + dx) % 4 * 12 + (y + dy) % 4 * 3 + i]
                        tile = wt[t, pl.ds(lo - i * TB, hi - lo)]
                        if dy == 0:
                            rbuf[k, 0, 0, 0, pl.ds(at, hi - lo)] = tile
                        else:
                            rsend[k, dy - 1, pl.ds(at, hi - lo)] = tile
                        at += hi - lo

    def stage_c(b):
        first, count = C_CH[b]
        for dz in range(4):
            for dc in range(2):
                for j in range(first, first + count):
                    t = tile_map[((z + dz) % 4 * 2 + (c + dc) % 2) * 6 + j]
                    if (dz, dc) == (0, 0):
                        cbuf[j, 0, 0] = wn[t]
                    else:
                        csend[j, dz * 2 + dc - 1] = wn[t]

    stage_r(0)
    stage_c(0)
    stage_r(1)
    stage_c(1)
    pl.semaphore_wait(barrier, len(places))

    partner = dev(dc=1)
    y_up, y_dn, z_up, z_dn = dev(dy=1), dev(dy=3), dev(dz=1), dev(dz=3)

    r_left, c_left = ("r", lambda: rsend), ("c", lambda: csend)
    r1_left, r2_left = ("r1", lambda: rbuf.at[0]), ("r2", lambda: rbuf.at[0, pl.ds(0, 2)])
    c1_left, c2_left = ("c1", lambda: cbuf.at[pl.ds(0, 3)]), ("c2", lambda: cbuf.at[pl.ds(0, 3), pl.ds(0, 2)])
    over_left = ("over", lambda: rbuf.at[pl.ds(0, 2)])

    def tiles(b):
        return pl.ds(*C_CH[b])

    def spread_r(k):
        arrival = (f"r{k}", lambda: rbuf.at[k, 0, 0, pl.ds(1, 3)])
        for d in (1, 3, 2):
            send(rsend.at[k, d - 1], rbuf.at[k, 0, 0, 4 - d], dev(dy=d), arrival, r_left)

    def spread_c(b):
        arrival = (f"c{b}", lambda: cbuf.at[tiles(b), 0, pl.ds(1, 7)])
        for dz, dc in line:
            src = csend.at[tiles(b), dz * 2 + dc - 1]
            send(src, cbuf.at[tiles(b), 0, (4 - dz) % 4 * 2 + dc], dev(dz=dz, dc=dc), arrival, c_left)

    def r_ref(k, rz, part):
        return rbuf.at[k, rz, 0, part]

    def c_ref(b, ry, part):
        return cbuf.at[tiles(b), ry, part]

    def gather1(ref, i, up, dn, halves, name, leaving):
        first, second = halves
        wait(got, f"{name}{i}")
        one, other = (f"{name}up{i}", lambda: ref(i, 3, first)), (f"{name}dn{i}", lambda: ref(i, 1, second))
        rest = (f"{name}rest{i}", lambda: ref(i, 1, pl.ds(0, 2 * first.size)))
        send(ref(i, 0, first), ref(i, 3, first), up, one, leaving)
        send(ref(i, 0, second), ref(i, 1, second), dn, other, leaving)
        send(ref(i, 0, second), ref(i, 3, second), up, rest, leaving)
        send(ref(i, 0, first), ref(i, 1, first), dn, rest, leaving)

    def gather2(ref, i, up, dn, halves, name, leaving):
        first, second = halves
        far = (f"{name}far{i}", lambda: ref(i, 2, pl.ds(0, 2 * first.size)))
        wait(got, f"{name}up{i}")
        send(ref(i, 3, first), ref(i, 2, first), up, far, leaving)
        wait(got, f"{name}dn{i}")
        send(ref(i, 1, second), ref(i, 2, second), dn, far, leaving)

    r_halves = (pl.ds(0, 2), pl.ds(2, 2))
    c_halves = (pl.ds(0, 4), pl.ds(4, 4))

    def over(k, rz):
        send(rbuf.at[k, rz, 0], rbuf.at[k, rz, 1], partner, (f"over{k}", lambda: rbuf.at[k, :, 1]), over_left)

    def r1(k):
        gather1(r_ref, k, z_up, z_dn, r_halves, "r", r1_left)
        over(k, 0)

    def r2(k):
        gather2(r_ref, k, z_up, z_dn, r_halves, "r", r2_left)

    def rd(k):
        wait(got, f"rrest{k}")
        over(k, 3)
        over(k, 1)

    def re(k):
        wait(got, f"rfar{k}")
        over(k, 2)

    def rf(k):
        wait(got, f"over{k}")

    def c1(b):
        gather1(c_ref, b, y_up, y_dn, c_halves, "c", c1_left)

    def c2(b):
        gather2(c_ref, b, y_up, y_dn, c_halves, "c", c2_left)

    def cf(b):
        wait(got, f"crest{b}")
        wait(got, f"cfar{b}")

    def pick(s, values):
        out = values[0]
        for i in range(1, len(values)):
            out = jnp.where(s == i, values[i], out)
        return out

    def block(s):
        k, j, j2 = (pick(s, [block[i] for block in ORDER]) for i in range(3))
        groups = [(rz, rc, ry) for rz in range(4) for rc in range(2) for ry in range(4)]
        lhs = jnp.concatenate([rbuf[k, rz, rc, ry] for rz, rc, ry in groups], axis=1)
        left = jnp.concatenate([cbuf[j, ry, rz * 2 + rc] for rz, rc, ry in groups], axis=0)
        right = jnp.concatenate([cbuf[j2, ry, rz * 2 + rc] for rz, rc, ry in groups], axis=0)
        value = jnp.dot(lhs, jnp.concatenate([left, right], axis=1), preferred_element_type=F32)
        last = k == NA - 1
        own[jnp.where(last, j, NJ)] = value[:, :TB]
        own[jnp.where(last, j2, NJ)] = value[:, TB:]
        rss[j, k] = value[:, :TB].astype(BF16)
        rss[j2, k] = value[:, TB:].astype(BF16)

        @pl.when(k == 0)
        def _():
            to = place(2, 0, 0, 0)
            reduce(j, k, 0, to).start()

            @pl.when(j2 > j)
            def _():
                reduce(j2, k, 0, to).start()

        @pl.when((k == 1) | (k == 2))
        def _():
            up, dn = place(1, 0, 0, 0), place(3, 0, 0, 0)
            reduce(j, k, 1, up).start()
            reduce(j, k, 3, dn).start()

            @pl.when(j2 > j)
            def _():
                reduce(j2, k, 1, up).start()
                reduce(j2, k, 3, dn).start()

    def reduce(j, k, dx, to):
        if dx == 0:
            src, dst = rss.at[j, k], rsr.at[j, 2]
        else:
            src = rss.at[j, k, pl.ds(192 * (dx // 2), 192)]
            dst = rsr.at[j, 4 - dx, pl.ds((k - 1) * 192, 192)]
        return pltpu.make_async_remote_copy(
            src_ref=src, dst_ref=dst, send_sem=sum_ssem, recv_sem=sum_rsem.at[j],
            device_id=to, device_id_type=MESH,
        )

    def small1():
        def partial(t, carry):
            part = jnp.dot(half, jnp.concatenate([wn[2 * t], wn[2 * t + 1]], axis=1), preferred_element_type=F32)
            for i in range(2):
                pall[2 * t + i] = part[0:1, i * TB : (i + 1) * TB]
            return carry

        lax.fori_loop(0, 24, partial, 0, unroll=6)
        for dy in range(4):
            for xx in range(4):
                for i in range(3):
                    t = tile_map[xx * 12 + (y + dy) % 4 * 3 + i]
                    psend[dy, xx, i : i + 1] = pall[t]
        o_in, o_out = (("o1", lambda: obs_all.at[r, pl.ds(0, 7)]),) * 2
        for dz, dc in line:
            send(obs_all.at[r, q], obs_all.at[r, q], dev(dz=dz, dc=dc), o_in, o_out)
        pbuf[y] = psend[0]
        p_in, p_out = ("p1", lambda: pbuf.at[pl.ds(0, 3)]), ("p1", lambda: psend.at[pl.ds(1, 3)])
        for d in (1, 2, 3):
            send(psend.at[d], pbuf.at[y], dev(dy=d), p_in, p_out)

    def small2():
        wait(got, "o1")
        wait(got, "p1")
        o_in, o_out = (("o2", lambda: obs_all.at[pl.ds(0, 3)]),) * 2
        for d in (1, 2, 3):
            send(obs_all.at[r], obs_all.at[r], dev(dy=d), o_in, o_out)
        qbuf[q] = (pbuf[0] + pbuf[1]) + (pbuf[2] + pbuf[3])
        p_in, p_out = (("p2", lambda: qbuf.at[pl.ds(0, 7)]),) * 2
        for dz, dc in line:
            send(qbuf.at[q], qbuf.at[q], dev(dz=dz, dc=dc), p_in, p_out)

    def small3():
        wait(got, "o2")
        wait(got, "p2")
        o_in, o_out = (("o3", lambda: obs_all.at[pl.ds(0, 12)]),) * 2
        for d in (1, 2, 3):
            send(obs_all.at[x_rows], obs_all.at[x_rows], dev(dx=d), o_in, o_out)
        total = qbuf[0]
        for i in range(1, 8):
            total = total + qbuf[i]
        tot[...] = total
        tbuf[x] = tot[x]
        p_in, p_out = ("p3", lambda: tbuf.at[pl.ds(0, 3)]), ("p3", lambda: tot.at[pl.ds(0, 3)])
        for d in (1, 2, 3):
            send(tot.at[x_of[d]], tbuf.at[x], dev(dx=d), p_in, p_out)

    def small4():
        wait(got, "o3")
        wait(got, "p3")
        rhs[...] = (tbuf[0] + tbuf[1]) + (tbuf[2] + tbuf[3])
        every = obs_all[...].reshape(16 * 8, 1, TB)
        block_of = lax.broadcasted_iota(jnp.int32, every.shape, 0)
        bal[...] = jnp.sum(jnp.where(block_of == plan[...], every, 0.0), axis=0)

    spread_r(0)
    spread_c(0)
    spread_r(1)
    spread_c(1)
    stage_r(2)
    stage_c(2)
    stage_r(3)
    stage_c(3)
    r1(0)
    c1(0)
    small1()
    r2(0)
    r1(1)
    c2(0)
    spread_r(2)
    spread_c(2)
    c1(1)
    rd(0)
    re(0)
    spread_r(3)
    spread_c(3)
    r2(1)
    r1(2)
    small2()
    rf(0)
    cf(0)
    c2(1)
    c1(2)

    def before1():
        rd(1)
        re(1)
        r2(2)
        r1(3)
        rf(1)

    def before2():
        c2(2)
        c1(3)
        cf(1)

    def before4():
        rd(2)
        re(2)
        r2(3)
        rf(2)

    def before6():
        cf(2)
        c2(3)

    def before8():
        rd(3)

    def before9():
        small3()
        re(3)
        cf(3)

    def before12():
        rf(3)

    acts = (
        (1, before1), (2, before2), (4, before4), (6, before6), (8, before8), (9, before9), (12, before12),
    )

    def slot(s, carry):
        for i, act in acts:
            pl.when(s == i)(act)
        block(s)
        return carry

    lax.fori_loop(0, len(ORDER), slot, 0)
    small4()
    for j in range(NJ):
        arrived = rsr.at[j, pl.ds(1, 3)]
        pltpu.make_async_copy(arrived, arrived, sum_rsem.at[j]).wait()
        total = own[j]
        for dx in (1, 2, 3):
            total = total + rsr[j, dx].astype(F32)
        gram[:, j * TB : (j + 1) * TB] = total
    for name in left:
        wait(left, name)
    sent = rss.at[:, pl.ds(0, 3)]
    pltpu.make_async_copy(sent, sent, sum_ssem).wait()


def on_device(
    design, observations, gaps, noise_var, arc_lengths, arc_amp, arc_decay, plan, tile_map
):
    smem = pl.BlockSpec(memory_space=pltpu.SMEM)
    vmem = pl.BlockSpec(memory_space=pltpu.VMEM)
    gram, rhs, bal = pl.pallas_call(
        kernel,
        name="normal_equations",
        out_shape=(
            pltpu.VMEM((384, 768), F32),
            pltpu.VMEM((3, TB), F32),
            pltpu.VMEM((1, TB), F32),
        ),
        in_specs=[smem] * 4 + [vmem] + [pl.BlockSpec(memory_space=pl.ANY)] * 4,
        out_specs=(vmem, vmem, vmem),
        scratch_shapes=[
            pltpu.VMEM((2, 1, TB), F32),
            pltpu.VMEM((1, TB), jnp.int32),
            pltpu.VMEM((TB, 6144), BF16),
            pltpu.VMEM((48, TB, TB), BF16),
            pltpu.VMEM((48, TB, TB), BF16),
            pltpu.VMEM((48, 1, TB), F32),
            pltpu.VMEM((NA, 4, 2, 4, 384, TB), BF16),
            pltpu.VMEM((NA, 3, 384, TB), BF16),
            pltpu.VMEM((NJ, 4, 8, TB, TB), BF16),
            pltpu.VMEM((NJ, 7, TB, TB), BF16),
            pltpu.VMEM((NJ + 1, 384, TB), F32),
            pltpu.VMEM((NJ, 4, 384, TB), BF16),
            pltpu.VMEM((NJ, 4, 384, TB), BF16),
            pltpu.VMEM((16, 8, 1, TB), F32),
            pltpu.VMEM((4, 4, 3, TB), F32),
            pltpu.VMEM((4, 4, 3, TB), F32),
            pltpu.VMEM((8, 4, 3, TB), F32),
            pltpu.VMEM((4, 3, TB), F32),
            pltpu.VMEM((4, 3, TB), F32),
            pltpu.SemaphoreType.DMA((4,)),
            pltpu.SemaphoreType.DMA((N_LEFT,)),
            pltpu.SemaphoreType.DMA((N_GOT,)),
            pltpu.SemaphoreType.DMA,
            pltpu.SemaphoreType.DMA((NJ,)),
        ],
        compiler_params=pltpu.CompilerParams(
            collective_id=0, has_side_effects=True, vmem_limit_bytes=60 * 1024 * 1024
        ),
    )(
        tile_map,
        arc_lengths,
        arc_amp,
        arc_decay,
        plan.reshape(1, 1),
        design,
        observations.reshape(1, TB),
        gaps.reshape(1, TB),
        noise_var.reshape(1, TB),
    )
    return gram, rhs.reshape(384), bal


def solution(mesh):
    placed = (
        P(("row", "col"), None),
        P(("row", "col")),
        P(("row", "col")),
        P(("row", "col")),
        P(("row", "col"), None),
        P(("row", "col"), None),
        P(("row", "col"), None),
        P(("row", "col")),
        P(),
    )
    return jax.shard_map(
        on_device,
        mesh=mesh,
        in_specs=placed,
        out_specs=(P("row", "col"), P("row"), P(("row", "col"), None)),
        check_vma=False,
    )
```

```python
import jax
import jax.numpy as jnp
from jax import lax
from jax.experimental import pallas as pl
from jax.experimental.pallas import tpu as pltpu
from jax.sharding import PartitionSpec as P

MESH = pl.DeviceIdType.MESH
F32 = jnp.float32
BF16 = jnp.bfloat16
TB = 128
R_CH = (((2, 0, 384),), ((1, 0, 192), (3, 0, 192)), ((1, 192, 192), (3, 192, 192)), ((0, 0, 384),))
C_CH = ((0, 2), (2, 2), (4, 1), (5, 1))
NA, NB, NJ = len(R_CH), len(C_CH), 6
ORDER = (
    (0, 0, 1), (1, 0, 1), (0, 2, 3), (1, 2, 3), (2, 0, 1), (2, 2, 3), (0, 4, 4), (1, 4, 4), (2, 4, 4),
    (0, 5, 5), (1, 5, 5), (2, 5, 5), (3, 0, 1), (3, 2, 3), (3, 4, 5),
)
N_GOT, N_LEFT = 50, 13


def inverse_factor(lens, amps, decays, gaps, noise, obs):
    shape = (8, TB)
    pos = lax.broadcasted_iota(jnp.int32, shape, 1)
    live = jnp.broadcast_to(gaps, shape).astype(F32)
    noise = jnp.broadcast_to(noise, shape)
    e0 = lens[0, 0]
    e1 = e0 + lens[0, 1]
    e2 = e1 + lens[0, 2]

    def by_arc(p, v):
        return jnp.where(p < e0, v[0], jnp.where(p < e1, v[1], jnp.where(p < e2, v[2], v[3])))

    amp = by_arc(pos, [amps[0, i] for i in range(4)])
    decay = by_arc(pos, [decays[0, i] for i in range(4)])
    start = (pos == 0) | (pos == e0) | (pos == e1) | (pos == e2)
    gain = decay * decay
    q = amp * (1.0 - gain)
    live_prev = pltpu.roll(live, 1, 1) > 0.5
    noise_prev = pltpu.roll(noise, 1, 1)
    a = jnp.where(start, 0.0, jnp.where(live_prev, gain * noise_prev + q, gain))
    b = jnp.where(start, amp, jnp.where(live_prev, q * noise_prev, q))
    c = jnp.where(start, 0.0, jnp.where(live_prev, 1.0, 0.0))
    d = jnp.where(start, 1.0, jnp.where(live_prev, noise_prev, 1.0))
    for shift in (1, 2, 4, 8, 16, 32):
        ok = pos >= shift
        ap, bp = pltpu.roll(a, shift, 1), pltpu.roll(b, shift, 1)
        cp, dp = pltpu.roll(c, shift, 1), pltpu.roll(d, shift, 1)
        an = jnp.where(ok, a * ap + b * cp, a)
        bn = jnp.where(ok, a * bp + b * dp, b)
        cn = jnp.where(ok, c * ap + d * cp, c)
        dn = jnp.where(ok, c * bp + d * dp, d)
        scale = 1.0 / (an + bn + cn + dn)
        a, b, c, d = an * scale, bn * scale, cn * scale, dn * scale
    var = b / d
    is_live = live > 0.5
    total = jnp.where(is_live, var, 0.0) + noise
    root = live * lax.rsqrt(total)
    log_step = jnp.log(jnp.where(is_live, decay * (noise / total), decay))
    push = jnp.where(is_live, decay * (var / total), 0.0)
    sq = (TB, TB)
    row = lax.broadcasted_iota(jnp.int32, sq, 0)
    col = lax.broadcasted_iota(jnp.int32, sq, 1)
    upto = (row <= col).astype(F32)
    cum = jnp.dot(log_step, upto, precision=lax.Precision.HIGHEST, preferred_element_type=F32)
    before = cum - log_step
    eye = row == col

    def as_column(v):
        return jnp.sum(jnp.where(eye, jnp.broadcast_to(v[0:1], sq), 0.0), axis=1, keepdims=True)

    def arc_of(p):
        return by_arc(p, [0, 1, 2, 3])

    inside = (row > col) & (arc_of(row) == arc_of(col))
    span = jnp.where(inside, as_column(before) - cum[0:1], -1e30)
    lower = jnp.where(eye, 1.0, -jnp.exp(span) * push[0:1])
    inv = as_column(root) * lower
    white_col = jnp.sum(inv * obs, axis=1, keepdims=True)
    white_row = jnp.sum(jnp.where(eye, white_col, 0.0), axis=0, keepdims=True)
    return inv, white_row


def kernel(
    tile_map, lens, amps, decays, plan, design, obs, gaps, noise,
    gram, rhs, bal,
    dbuf, wn, wt, pall, rbuf, rsend, cbuf, csend, own, rss, rsr, obs_all, psend, pbuf, qbuf, tot, tbuf,
    load_sem, ssem, rsem, sum_ssem, sum_rsem,
):
    r, q = lax.axis_index("row"), lax.axis_index("col")
    x, y, z, c = r // 4, r % 4, q // 2, q % 2

    def place(dx, dy, dz, dc):
        return ((x + dx) % 4 * 4 + (y + dy) % 4, (z + dz) % 4 * 2 + (c + dc) % 2)

    steps = [(i, 0, 0, 0) for i in (1, 2, 3)] + [(0, i, 0, 0) for i in (1, 2, 3)]
    steps = steps + [(0, 0, i, j) for i in range(4) for j in range(2) if (i, j) != (0, 0)]
    places = {step: place(*step) for step in steps}

    def dev(dx=0, dy=0, dz=0, dc=0):
        return places[dx, dy, dz, dc]

    x_of = [(x + d) % 4 for d in range(4)]
    x_rows = pl.ds(4 * x, 4)

    got, left = {}, {}

    def group(table, sems, name, region):
        if name not in table:
            table[name] = (len(table), sems, region)
        return table[name][0]

    def wait(table, name):
        i, sems, region = table[name]
        pltpu.make_async_copy(region(), region(), sems.at[i]).wait()

    def send(src, dst, to, arrival, leaving):
        pltpu.make_async_remote_copy(
            src_ref=src, dst_ref=dst, send_sem=ssem.at[group(left, ssem, *leaving)], recv_sem=rsem.at[group(got, rsem, *arrival)],
            device_id=to, device_id_type=MESH,
        ).start()

    for t in range(48):
        pltpu.make_async_copy(design.at[:, pl.ds(t * TB, TB)], dbuf.at[t], load_sem).start()
    line = [(dz, dc) for dz in range(4) for dc in range(2) if (dz, dc) != (0, 0)]
    barrier = pltpu.get_barrier_semaphore()
    for p in places.values():
        pl.semaphore_signal(barrier, inc=1, device_id=p, device_id_type=MESH)

    inv, white_row = inverse_factor(lens, amps, decays, gaps[...], noise[...], obs[...])
    hi = inv.astype(BF16)
    lo = (inv - hi.astype(F32)).astype(BF16)
    both = jnp.concatenate([hi, lo], axis=1)
    obs_all[r, q] = white_row
    half = jnp.broadcast_to(white_row, (8, TB)).astype(BF16)
    pltpu.make_async_copy(dbuf, dbuf, load_sem).wait()

    def whitened(cols):
        return jnp.dot(both, jnp.concatenate([cols, cols], axis=0), preferred_element_type=F32)

    def slot_pair(s, s2):
        cols = [dbuf[tile_map[i]] for i in (s, s2)]
        return whitened(jnp.concatenate(cols, axis=1))

    def whiten_pair(t, carry):
        white = whitened(jnp.concatenate([dbuf[2 * t], dbuf[2 * t + 1]], axis=1))
        kept = white.astype(BF16)
        flipped = white.T.astype(BF16)
        for i in range(2):
            wn[2 * t + i] = kept[:, i * TB : (i + 1) * TB]
            wt[2 * t + i] = flipped[i * TB : (i + 1) * TB]
        return carry


    def stage_r(k):
        for dy in range(4):
            at = 0
            for dx, first, count in R_CH[k]:
                for i in range(3):
                    lo, hi = max(first, i * TB), min(first + count, i * TB + TB)
                    if lo < hi:
                        t = tile_map[(x + dx) % 4 * 12 + (y + dy) % 4 * 3 + i]
                        tile = wt[t, pl.ds(lo - i * TB, hi - lo)]
                        if dy == 0:
                            rbuf[k, 0, 0, 0, pl.ds(at, hi - lo)] = tile
                        else:
                            rsend[k, dy - 1, pl.ds(at, hi - lo)] = tile
                        at += hi - lo

    def stage_c(b):
        first, count = C_CH[b]
        for dz in range(4):
            for dc in range(2):
                for j in range(first, first + count):
                    t = tile_map[((z + dz) % 4 * 2 + (c + dc) % 2) * 6 + j]
                    if (dz, dc) == (0, 0):
                        cbuf[j, 0, 0] = wn[t]
                    else:
                        csend[j, dz * 2 + dc - 1] = wn[t]

    partner = dev(dc=1)
    y_up, y_dn, z_up, z_dn = dev(dy=1), dev(dy=3), dev(dz=1), dev(dz=3)

    r_left, c_left = ("r", lambda: rsend), ("c", lambda: csend)
    r1_left, r2_left = ("r1", lambda: rbuf.at[0]), ("r2", lambda: rbuf.at[0, pl.ds(0, 2)])
    c1_left, c2_left = ("c1", lambda: cbuf.at[pl.ds(0, 3)]), ("c2", lambda: cbuf.at[pl.ds(0, 3), pl.ds(0, 2)])
    over_left = ("over", lambda: rbuf.at[pl.ds(0, 2)])

    def tiles(b):
        return pl.ds(*C_CH[b])

    def spread_r(k):
        arrival = (f"r{k}", lambda: rbuf.at[k, 0, 0, pl.ds(1, 3)])
        for d in (1, 3, 2):
            send(rsend.at[k, d - 1], rbuf.at[k, 0, 0, 4 - d], dev(dy=d), arrival, r_left)

    def spread_c(b):
        arrival = (f"c{b}", lambda: cbuf.at[tiles(b), 0, pl.ds(1, 7)])
        for dz, dc in line:
            src = csend.at[tiles(b), dz * 2 + dc - 1]
            send(src, cbuf.at[tiles(b), 0, (4 - dz) % 4 * 2 + dc], dev(dz=dz, dc=dc), arrival, c_left)

    def r_ref(k, rz, part):
        return rbuf.at[k, rz, 0, part]

    def c_ref(b, ry, part):
        return cbuf.at[tiles(b), ry, part]

    def pieces(part):
        return [pl.ds(i, 1) for i in range(part.start, part.start + part.size)]

    def gather1(ref, i, up, dn, halves, name, leaving):
        first, second = halves
        wait(got, f"{name}{i}")
        one, other = (f"{name}up{i}", lambda: ref(i, 3, first)), (f"{name}dn{i}", lambda: ref(i, 1, second))
        rest = (f"{name}rest{i}", lambda: ref(i, 1, pl.ds(0, 2 * first.size)))
        for p, p2 in zip(pieces(first), pieces(second)):
            send(ref(i, 0, p), ref(i, 3, p), up, one, leaving)
            send(ref(i, 0, p2), ref(i, 1, p2), dn, other, leaving)
        send(ref(i, 0, second), ref(i, 3, second), up, rest, leaving)
        send(ref(i, 0, first), ref(i, 1, first), dn, rest, leaving)

    def gather2(ref, i, up, dn, halves, name, leaving):
        first, second = halves
        far = (f"{name}far{i}", lambda: ref(i, 2, pl.ds(0, 2 * first.size)))
        wait(got, f"{name}up{i}")
        for p in pieces(first):
            send(ref(i, 3, p), ref(i, 2, p), up, far, leaving)
        wait(got, f"{name}dn{i}")
        for p in pieces(second):
            send(ref(i, 1, p), ref(i, 2, p), dn, far, leaving)

    r_halves = (pl.ds(0, 2), pl.ds(2, 2))
    c_halves = (pl.ds(0, 4), pl.ds(4, 4))

    def over(k, rz):
        send(rbuf.at[k, rz, 0], rbuf.at[k, rz, 1], partner, (f"over{k}", lambda: rbuf.at[k, :, 1]), over_left)

    def r1(k):
        gather1(r_ref, k, z_up, z_dn, r_halves, "r", r1_left)
        over(k, 0)

    def r2(k):
        gather2(r_ref, k, z_up, z_dn, r_halves, "r", r2_left)

    def rd(k):
        wait(got, f"rrest{k}")
        over(k, 3)
        over(k, 1)

    def re(k):
        wait(got, f"rfar{k}")
        over(k, 2)

    def rf(k):
        wait(got, f"over{k}")

    def c1(b):
        gather1(c_ref, b, y_up, y_dn, c_halves, "c", c1_left)

    def c2(b):
        gather2(c_ref, b, y_up, y_dn, c_halves, "c", c2_left)

    def cf(b):
        wait(got, f"crest{b}")
        wait(got, f"cfar{b}")

    def pick(s, values):
        out = values[0]
        for i in range(1, len(values)):
            out = jnp.where(s == i, values[i], out)
        return out

    def block(s):
        k, j, j2 = (pick(s, [block[i] for block in ORDER]) for i in range(3))
        groups = [(rz, rc, ry) for rz in range(4) for rc in range(2) for ry in range(4)]
        lhs = jnp.concatenate([rbuf[k, rz, rc, ry] for rz, rc, ry in groups], axis=1)
        left = jnp.concatenate([cbuf[j, ry, rz * 2 + rc] for rz, rc, ry in groups], axis=0)
        right = jnp.concatenate([cbuf[j2, ry, rz * 2 + rc] for rz, rc, ry in groups], axis=0)
        value = jnp.dot(lhs, jnp.concatenate([left, right], axis=1), preferred_element_type=F32)
        last = k == NA - 1
        own[jnp.where(last, j, NJ)] = value[:, :TB]
        own[jnp.where(last, j2, NJ)] = value[:, TB:]
        rss[j, k] = value[:, :TB].astype(BF16)
        rss[j2, k] = value[:, TB:].astype(BF16)

        @pl.when(k == 0)
        def _():
            to = place(2, 0, 0, 0)
            reduce(j, k, 0, to).start()

            @pl.when(j2 > j)
            def _():
                reduce(j2, k, 0, to).start()

        @pl.when((k == 1) | (k == 2))
        def _():
            up, dn = place(1, 0, 0, 0), place(3, 0, 0, 0)
            reduce(j, k, 1, up).start()
            reduce(j, k, 3, dn).start()

            @pl.when(j2 > j)
            def _():
                reduce(j2, k, 1, up).start()
                reduce(j2, k, 3, dn).start()

    def reduce(j, k, dx, to):
        if dx == 0:
            src, dst = rss.at[j, k], rsr.at[j, 2]
        else:
            src = rss.at[j, k, pl.ds(192 * (dx // 2), 192)]
            dst = rsr.at[j, 4 - dx, pl.ds((k - 1) * 192, 192)]
        return pltpu.make_async_remote_copy(
            src_ref=src, dst_ref=dst, send_sem=sum_ssem, recv_sem=sum_rsem.at[j],
            device_id=to, device_id_type=MESH,
        )

    def small1():
        def partial(t, carry):
            part = jnp.dot(half, jnp.concatenate([wn[2 * t], wn[2 * t + 1]], axis=1), preferred_element_type=F32)
            for i in range(2):
                pall[2 * t + i] = part[0:1, i * TB : (i + 1) * TB]
            return carry

        lax.fori_loop(0, 24, partial, 0, unroll=6)
        for dy in range(4):
            for xx in range(4):
                for i in range(3):
                    t = tile_map[xx * 12 + (y + dy) % 4 * 3 + i]
                    psend[dy, xx, i : i + 1] = pall[t]
        o_in, o_out = (("o1", lambda: obs_all.at[r, pl.ds(0, 7)]),) * 2
        for dz, dc in line:
            send(obs_all.at[r, q], obs_all.at[r, q], dev(dz=dz, dc=dc), o_in, o_out)
        pbuf[y] = psend[0]
        p_in, p_out = ("p1", lambda: pbuf.at[pl.ds(0, 3)]), ("p1", lambda: psend.at[pl.ds(1, 3)])
        for d in (1, 2, 3):
            send(psend.at[d], pbuf.at[y], dev(dy=d), p_in, p_out)

    def small2():
        wait(got, "o1")
        wait(got, "p1")
        o_in, o_out = (("o2", lambda: obs_all.at[pl.ds(0, 3)]),) * 2
        for d in (1, 2, 3):
            send(obs_all.at[r], obs_all.at[r], dev(dy=d), o_in, o_out)
        qbuf[q] = (pbuf[0] + pbuf[1]) + (pbuf[2] + pbuf[3])
        p_in, p_out = (("p2", lambda: qbuf.at[pl.ds(0, 7)]),) * 2
        for dz, dc in line:
            send(qbuf.at[q], qbuf.at[q], dev(dz=dz, dc=dc), p_in, p_out)

    def small3():
        wait(got, "o2")
        wait(got, "p2")
        o_in, o_out = (("o3", lambda: obs_all.at[pl.ds(0, 12)]),) * 2
        for d in (1, 2, 3):
            send(obs_all.at[x_rows], obs_all.at[x_rows], dev(dx=d), o_in, o_out)
        total = qbuf[0]
        for i in range(1, 8):
            total = total + qbuf[i]
        tot[...] = total
        tbuf[x] = tot[x]
        p_in, p_out = ("p3", lambda: tbuf.at[pl.ds(0, 3)]), ("p3", lambda: tot.at[pl.ds(0, 3)])
        for d in (1, 2, 3):
            send(tot.at[x_of[d]], tbuf.at[x], dev(dx=d), p_in, p_out)

    def small4():
        wait(got, "o3")
        wait(got, "p3")
        rhs[...] = (tbuf[0] + tbuf[1]) + (tbuf[2] + tbuf[3])
        every = obs_all[...].reshape(16 * 8, 1, TB)
        block_of = lax.broadcasted_iota(jnp.int32, every.shape, 0)
        bal[...] = jnp.sum(jnp.where(block_of == plan[...], every, 0.0), axis=0)

    first_r = [(dy, i) for dy in (1, 2, 3, 0) for i in range(3)]
    for n in range(0, 12, 2):
        pair = first_r[n : n + 2]
        white = slot_pair(*[(x + R_CH[0][0][0]) % 4 * 12 + (y + dy) % 4 * 3 + i for dy, i in pair])
        flipped = white.T.astype(BF16)
        for m, (dy, i) in enumerate(pair):
            tile, rows = flipped[m * TB : (m + 1) * TB], pl.ds(i * TB, TB)
            if dy == 0:
                rbuf[0, 0, 0, 0, rows] = tile
            else:
                rsend[0, dy - 1, rows] = tile
    pl.semaphore_wait(barrier, len(places))
    spread_r(0)
    for dz, dc in line + [(0, 0)]:
        base = ((z + dz) % 4 * 2 + (c + dc) % 2) * 6
        white = slot_pair(base, base + 1).astype(BF16)
        for j in range(2):
            tile = white[:, j * TB : (j + 1) * TB]
            if (dz, dc) == (0, 0):
                cbuf[j, 0, 0] = tile
            else:
                csend[j, dz * 2 + dc - 1] = tile
    spread_c(0)
    lax.fori_loop(0, 24, whiten_pair, 0, unroll=6)
    stage_r(1)
    stage_c(1)
    spread_r(1)
    spread_c(1)
    stage_r(2)
    stage_c(2)
    stage_r(3)
    stage_c(3)
    r1(0)
    c1(0)
    small1()
    r2(0)
    r1(1)
    c2(0)
    spread_r(2)
    spread_c(2)
    c1(1)
    rd(0)
    re(0)
    r2(1)
    r1(2)
    spread_c(3)
    spread_r(3)
    small2()
    rf(0)
    cf(0)
    c2(1)

    def before1():
        rd(1)
        re(1)
        c1(2)
        r2(2)
        r1(3)
        rf(1)

    def before2():
        cf(1)

    def before4():
        c2(2)
        c1(3)
        rd(2)
        re(2)
        rf(2)

    def before6():
        r2(3)
        cf(2)

    def before8():
        c2(3)
        rd(3)

    def before9():
        small3()
        re(3)
        cf(3)

    def before12():
        rf(3)

    acts = (
        (1, before1), (2, before2), (4, before4), (6, before6), (8, before8), (9, before9), (12, before12),
    )

    def slot(s, carry):
        for i, act in acts:
            pl.when(s == i)(act)
        block(s)
        return carry

    lax.fori_loop(0, len(ORDER), slot, 0)
    small4()
    for j in range(NJ):
        arrived = rsr.at[j, pl.ds(1, 3)]
        pltpu.make_async_copy(arrived, arrived, sum_rsem.at[j]).wait()
        total = own[j]
        for dx in (1, 2, 3):
            total = total + rsr[j, dx].astype(F32)
        gram[:, j * TB : (j + 1) * TB] = total
    for name in left:
        wait(left, name)
    sent = rss.at[:, pl.ds(0, 3)]
    pltpu.make_async_copy(sent, sent, sum_ssem).wait()


def hand_over(gram, rhs, bal, gram_out, rhs_out, bal_out, flat, sem):
    for i in range(3):
        flat[i * TB : (i + 1) * TB] = rhs[i]
    pairs = ((gram, gram_out), (bal, bal_out), (flat, rhs_out))
    copies = [pltpu.make_async_copy(src, dst, sem.at[i]) for i, (src, dst) in enumerate(pairs)]
    for cp in copies:
        cp.start()
    for cp in copies:
        cp.wait()


def on_device(
    design, observations, gaps, noise_var, arc_lengths, arc_amp, arc_decay, plan, tile_map
):
    smem = pl.BlockSpec(memory_space=pltpu.SMEM)
    vmem = pl.BlockSpec(memory_space=pltpu.VMEM)
    gram, rhs, bal = pl.pallas_call(
        kernel,
        name="normal_equations",
        out_shape=(
            pltpu.VMEM((384, 768), F32),
            pltpu.VMEM((3, TB), F32),
            pltpu.VMEM((1, TB), F32),
        ),
        in_specs=[smem] * 4 + [vmem, pl.BlockSpec(memory_space=pl.ANY)] + [vmem] * 3,
        out_specs=(vmem, vmem, vmem),
        scratch_shapes=[
            pltpu.VMEM((48, TB, TB), BF16),
            pltpu.VMEM((48, TB, TB), BF16),
            pltpu.VMEM((48, TB, TB), BF16),
            pltpu.VMEM((48, 1, TB), F32),
            pltpu.VMEM((NA, 4, 2, 4, 384, TB), BF16),
            pltpu.VMEM((NA, 3, 384, TB), BF16),
            pltpu.VMEM((NJ, 4, 8, TB, TB), BF16),
            pltpu.VMEM((NJ, 7, TB, TB), BF16),
            pltpu.VMEM((NJ + 1, 384, TB), F32),
            pltpu.VMEM((NJ, 4, 384, TB), BF16),
            pltpu.VMEM((NJ, 4, 384, TB), BF16),
            pltpu.VMEM((16, 8, 1, TB), F32),
            pltpu.VMEM((4, 4, 3, TB), F32),
            pltpu.VMEM((4, 4, 3, TB), F32),
            pltpu.VMEM((8, 4, 3, TB), F32),
            pltpu.VMEM((4, 3, TB), F32),
            pltpu.VMEM((4, 3, TB), F32),
            pltpu.SemaphoreType.DMA,
            pltpu.SemaphoreType.DMA((N_LEFT,)),
            pltpu.SemaphoreType.DMA((N_GOT,)),
            pltpu.SemaphoreType.DMA,
            pltpu.SemaphoreType.DMA((NJ,)),
        ],
        compiler_params=pltpu.CompilerParams(
            collective_id=0, has_side_effects=True, vmem_limit_bytes=60 * 1024 * 1024
        ),
    )(
        tile_map,
        arc_lengths,
        arc_amp,
        arc_decay,
        plan.reshape(1, 1),
        design,
        observations.reshape(1, TB),
        gaps.reshape(1, TB),
        noise_var.reshape(1, TB),
    )
    inner = [pltpu.with_memory_space_constraint(v, pltpu.VMEM) for v in (gram, rhs, bal)]
    anywhere = pl.BlockSpec(memory_space=pl.ANY)
    return pl.pallas_call(
        hand_over,
        name="hand_over",
        out_shape=(
            jax.ShapeDtypeStruct((384, 768), F32),
            jax.ShapeDtypeStruct((384,), F32),
            jax.ShapeDtypeStruct((1, TB), F32),
        ),
        in_specs=[vmem] * 3,
        out_specs=(anywhere, anywhere, anywhere),
        scratch_shapes=[pltpu.VMEM((384,), F32), pltpu.SemaphoreType.DMA((3,))],
        compiler_params=pltpu.CompilerParams(vmem_limit_bytes=1024 * 1024),
    )(*inner)


def solution(mesh):
    placed = (
        P(("row", "col"), None),
        P(("row", "col")),
        P(("row", "col")),
        P(("row", "col")),
        P(("row", "col"), None),
        P(("row", "col"), None),
        P(("row", "col"), None),
        P(("row", "col")),
        P(),
    )
    return jax.shard_map(
        on_device,
        mesh=mesh,
        in_specs=placed,
        out_specs=(P("row", "col"), P("row"), P(("row", "col"), None)),
        check_vma=False,
    )
```

```python
import jax
import jax.numpy as jnp
from jax import lax
from jax.experimental import pallas as pl
from jax.experimental.pallas import tpu as pltpu
from jax.sharding import PartitionSpec as P

MESH = pl.DeviceIdType.MESH
F32 = jnp.float32
BF16 = jnp.bfloat16
TB = 128
R_CH = (((2, 0, 384),), ((1, 0, 192), (3, 0, 192)), ((1, 192, 192), (3, 192, 192)), ((0, 0, 384),))
C_CH = ((0, 2), (2, 2), (4, 1), (5, 1))
NA, NB, NJ = len(R_CH), len(C_CH), 6
ORDER = (
    (0, 0, 1), (1, 0, 1), (0, 2, 3), (1, 2, 3), (2, 0, 1), (2, 2, 3), (0, 4, 4), (1, 4, 4), (2, 4, 4),
    (0, 5, 5), (1, 5, 5), (2, 5, 5), (3, 0, 1), (3, 2, 3), (3, 4, 5),
)
N_GOT, N_LEFT = 50, 13


def inverse_factor(lens, amps, decays, gaps, noise, obs):
    shape = (8, TB)
    pos = lax.broadcasted_iota(jnp.int32, shape, 1)
    live = jnp.broadcast_to(gaps, shape).astype(F32)
    noise = jnp.broadcast_to(noise, shape)
    e0 = lens[0, 0]
    e1 = e0 + lens[0, 1]
    e2 = e1 + lens[0, 2]

    def by_arc(p, v):
        return jnp.where(p < e0, v[0], jnp.where(p < e1, v[1], jnp.where(p < e2, v[2], v[3])))

    amp = by_arc(pos, [amps[0, i] for i in range(4)])
    decay = by_arc(pos, [decays[0, i] for i in range(4)])
    start = (pos == 0) | (pos == e0) | (pos == e1) | (pos == e2)
    gain = decay * decay
    q = amp * (1.0 - gain)
    live_prev = pltpu.roll(live, 1, 1) > 0.5
    noise_prev = pltpu.roll(noise, 1, 1)
    a = jnp.where(start, 0.0, jnp.where(live_prev, gain * noise_prev + q, gain))
    b = jnp.where(start, amp, jnp.where(live_prev, q * noise_prev, q))
    c = jnp.where(start, 0.0, jnp.where(live_prev, 1.0, 0.0))
    d = jnp.where(start, 1.0, jnp.where(live_prev, noise_prev, 1.0))
    for shift in (1, 2, 4, 8, 16, 32):
        ok = pos >= shift
        ap, bp = pltpu.roll(a, shift, 1), pltpu.roll(b, shift, 1)
        cp, dp = pltpu.roll(c, shift, 1), pltpu.roll(d, shift, 1)
        an = jnp.where(ok, a * ap + b * cp, a)
        bn = jnp.where(ok, a * bp + b * dp, b)
        cn = jnp.where(ok, c * ap + d * cp, c)
        dn = jnp.where(ok, c * bp + d * dp, d)
        if shift == 8:
            scale = 1.0 / (an + bn + cn + dn)
            an, bn, cn, dn = an * scale, bn * scale, cn * scale, dn * scale
        a, b, c, d = an, bn, cn, dn
    var = b / d
    is_live = live > 0.5
    total = jnp.where(is_live, var, 0.0) + noise
    root = live * lax.rsqrt(total)
    log_step = jnp.log(jnp.where(is_live, decay * (noise / total), decay))
    push = jnp.where(is_live, decay * (var / total), 0.0)
    sq = (TB, TB)
    row = lax.broadcasted_iota(jnp.int32, sq, 0)
    col = lax.broadcasted_iota(jnp.int32, sq, 1)
    upto = (row <= col).astype(F32)
    cum = jnp.dot(log_step, upto, precision=lax.Precision.HIGHEST, preferred_element_type=F32)
    before = cum - log_step
    eye = row == col

    def as_column(v):
        return jnp.sum(jnp.where(eye, jnp.broadcast_to(v[0:1], sq), 0.0), axis=1, keepdims=True)

    def arc_of(p):
        return by_arc(p, [0, 1, 2, 3])

    inside = (row > col) & (arc_of(row) == arc_of(col))
    span = jnp.where(inside, as_column(before) - cum[0:1], -1e30)
    lower = jnp.where(eye, 1.0, -jnp.exp(span) * push[0:1])
    inv = as_column(root) * lower
    white_col = jnp.sum(inv * obs, axis=1, keepdims=True)
    white_row = jnp.sum(jnp.where(eye, white_col, 0.0), axis=0, keepdims=True)
    return inv, white_row


def kernel(
    tile_map, lens, amps, decays, plan, design, obs, gaps, noise,
    gram, rhs, bal,
    dbuf, wn, wt, pall, rbuf, rsend, cbuf, csend, own, rss, rsr, obs_all, psend, pbuf, qbuf, tot, tbuf,
    load_sem, ssem, rsem, sum_ssem, sum_rsem,
):
    r, q = lax.axis_index("row"), lax.axis_index("col")
    x, y, z, c = r // 4, r % 4, q // 2, q % 2

    def place(dx, dy, dz, dc):
        return ((x + dx) % 4 * 4 + (y + dy) % 4, (z + dz) % 4 * 2 + (c + dc) % 2)

    steps = [(i, 0, 0, 0) for i in (1, 2, 3)] + [(0, i, 0, 0) for i in (1, 2, 3)]
    steps = steps + [(0, 0, i, j) for i in range(4) for j in range(2) if (i, j) != (0, 0)]
    places = {step: place(*step) for step in steps}

    def dev(dx=0, dy=0, dz=0, dc=0):
        return places[dx, dy, dz, dc]

    x_of = [(x + d) % 4 for d in range(4)]
    x_rows = pl.ds(4 * x, 4)

    got, left = {}, {}

    def group(table, sems, name, region):
        if name not in table:
            table[name] = (len(table), sems, region)
        return table[name][0]

    def wait(table, name):
        i, sems, region = table[name]
        pltpu.make_async_copy(region(), region(), sems.at[i]).wait()

    def send(src, dst, to, arrival, leaving):
        pltpu.make_async_remote_copy(
            src_ref=src, dst_ref=dst, send_sem=ssem.at[group(left, ssem, *leaving)], recv_sem=rsem.at[group(got, rsem, *arrival)],
            device_id=to, device_id_type=MESH,
        ).start()

    for t in range(48):
        pltpu.make_async_copy(design.at[:, pl.ds(t * TB, TB)], dbuf.at[t], load_sem).start()
    line = [(dz, dc) for dz in range(4) for dc in range(2) if (dz, dc) != (0, 0)]
    barrier = pltpu.get_barrier_semaphore()
    for p in places.values():
        pl.semaphore_signal(barrier, inc=1, device_id=p, device_id_type=MESH)

    inv, white_row = inverse_factor(lens, amps, decays, gaps[...], noise[...], obs[...])
    hi = inv.astype(BF16)
    lo = (inv - hi.astype(F32)).astype(BF16)
    both = jnp.concatenate([hi, lo], axis=1)
    obs_all[r, q] = white_row
    half = jnp.broadcast_to(white_row, (8, TB)).astype(BF16)
    pltpu.make_async_copy(dbuf, dbuf, load_sem).wait()

    def whitened(cols):
        return jnp.dot(both, jnp.concatenate([cols, cols], axis=0), preferred_element_type=F32)

    def slot_pair(s, s2):
        cols = [dbuf[tile_map[i]] for i in (s, s2)]
        return whitened(jnp.concatenate(cols, axis=1))

    def whiten_pair(t, carry):
        white = whitened(jnp.concatenate([dbuf[2 * t], dbuf[2 * t + 1]], axis=1))
        kept = white.astype(BF16)
        flipped = white.T.astype(BF16)
        for i in range(2):
            wn[2 * t + i] = kept[:, i * TB : (i + 1) * TB]
            wt[2 * t + i] = flipped[i * TB : (i + 1) * TB]
        return carry


    def stage_r(k):
        for dy in range(4):
            at = 0
            for dx, first, count in R_CH[k]:
                for i in range(3):
                    lo, hi = max(first, i * TB), min(first + count, i * TB + TB)
                    if lo < hi:
                        t = tile_map[(x + dx) % 4 * 12 + (y + dy) % 4 * 3 + i]
                        tile = wt[t, pl.ds(lo - i * TB, hi - lo)]
                        if dy == 0:
                            rbuf[k, 0, 0, 0, pl.ds(at, hi - lo)] = tile
                        else:
                            rsend[k, dy - 1, pl.ds(at, hi - lo)] = tile
                        at += hi - lo

    def stage_c(b):
        first, count = C_CH[b]
        for dz in range(4):
            for dc in range(2):
                for j in range(first, first + count):
                    t = tile_map[((z + dz) % 4 * 2 + (c + dc) % 2) * 6 + j]
                    if (dz, dc) == (0, 0):
                        cbuf[j, 0, 0] = wn[t]
                    else:
                        csend[j, dz * 2 + dc - 1] = wn[t]

    partner = dev(dc=1)
    y_up, y_dn, z_up, z_dn = dev(dy=1), dev(dy=3), dev(dz=1), dev(dz=3)

    r_left, c_left = ("r", lambda: rsend), ("c", lambda: csend)
    r1_left, r2_left = ("r1", lambda: rbuf.at[0]), ("r2", lambda: rbuf.at[0, pl.ds(0, 2)])
    c1_left, c2_left = ("c1", lambda: cbuf.at[pl.ds(0, 3)]), ("c2", lambda: cbuf.at[pl.ds(0, 3), pl.ds(0, 2)])
    over_left = ("over", lambda: rbuf.at[pl.ds(0, 2)])

    def tiles(b):
        return pl.ds(*C_CH[b])

    def spread_r(k):
        arrival = (f"r{k}", lambda: rbuf.at[k, 0, 0, pl.ds(1, 3)])
        for d in (1, 3, 2):
            send(rsend.at[k, d - 1], rbuf.at[k, 0, 0, 4 - d], dev(dy=d), arrival, r_left)

    def spread_c(b):
        arrival = (f"c{b}", lambda: cbuf.at[tiles(b), 0, pl.ds(1, 7)])
        for dz, dc in line:
            src = csend.at[tiles(b), dz * 2 + dc - 1]
            send(src, cbuf.at[tiles(b), 0, (4 - dz) % 4 * 2 + dc], dev(dz=dz, dc=dc), arrival, c_left)

    def r_ref(k, rz, part):
        return rbuf.at[k, rz, 0, part]

    def c_ref(b, ry, part):
        return cbuf.at[tiles(b), ry, part]

    def pieces(part):
        return [pl.ds(i, 1) for i in range(part.start, part.start + part.size)]

    def gather1(ref, i, up, dn, halves, name, leaving):
        first, second = halves
        wait(got, f"{name}{i}")
        one, other = (f"{name}up{i}", lambda: ref(i, 3, first)), (f"{name}dn{i}", lambda: ref(i, 1, second))
        rest = (f"{name}rest{i}", lambda: ref(i, 1, pl.ds(0, 2 * first.size)))
        for p, p2 in zip(pieces(first), pieces(second)):
            send(ref(i, 0, p), ref(i, 3, p), up, one, leaving)
            send(ref(i, 0, p2), ref(i, 1, p2), dn, other, leaving)
        send(ref(i, 0, second), ref(i, 3, second), up, rest, leaving)
        send(ref(i, 0, first), ref(i, 1, first), dn, rest, leaving)

    def gather2(ref, i, up, dn, halves, name, leaving):
        first, second = halves
        far = (f"{name}far{i}", lambda: ref(i, 2, pl.ds(0, 2 * first.size)))
        wait(got, f"{name}up{i}")
        for p in pieces(first):
            send(ref(i, 3, p), ref(i, 2, p), up, far, leaving)
        wait(got, f"{name}dn{i}")
        for p in pieces(second):
            send(ref(i, 1, p), ref(i, 2, p), dn, far, leaving)

    r_halves = (pl.ds(0, 2), pl.ds(2, 2))
    c_halves = (pl.ds(0, 4), pl.ds(4, 4))

    def over(k, rz):
        send(rbuf.at[k, rz, 0], rbuf.at[k, rz, 1], partner, (f"over{k}", lambda: rbuf.at[k, :, 1]), over_left)

    def r1(k):
        gather1(r_ref, k, z_up, z_dn, r_halves, "r", r1_left)
        over(k, 0)

    def r2(k):
        gather2(r_ref, k, z_up, z_dn, r_halves, "r", r2_left)

    def rd(k):
        wait(got, f"rrest{k}")
        over(k, 3)
        over(k, 1)

    def re(k):
        wait(got, f"rfar{k}")
        over(k, 2)

    def rf(k):
        wait(got, f"over{k}")

    def c1(b):
        gather1(c_ref, b, y_up, y_dn, c_halves, "c", c1_left)

    def c2(b):
        gather2(c_ref, b, y_up, y_dn, c_halves, "c", c2_left)

    def cf(b):
        wait(got, f"crest{b}")
        wait(got, f"cfar{b}")

    def pick(s, values):
        out = values[0]
        for i in range(1, len(values)):
            out = jnp.where(s == i, values[i], out)
        return out

    def block(s):
        k, j, j2 = (pick(s, [block[i] for block in ORDER]) for i in range(3))
        groups = [(rz, rc, ry) for rz in range(4) for rc in range(2) for ry in range(4)]
        lhs = jnp.concatenate([rbuf[k, rz, rc, ry] for rz, rc, ry in groups], axis=1)
        left = jnp.concatenate([cbuf[j, ry, rz * 2 + rc] for rz, rc, ry in groups], axis=0)
        right = jnp.concatenate([cbuf[j2, ry, rz * 2 + rc] for rz, rc, ry in groups], axis=0)
        value = jnp.dot(lhs, jnp.concatenate([left, right], axis=1), preferred_element_type=F32)
        last = k == NA - 1
        own[jnp.where(last, j, NJ)] = value[:, :TB]
        own[jnp.where(last, j2, NJ)] = value[:, TB:]
        rss[j, k] = value[:, :TB].astype(BF16)
        rss[j2, k] = value[:, TB:].astype(BF16)

        @pl.when(k == 0)
        def _():
            to = place(2, 0, 0, 0)
            reduce(j, k, 0, to).start()

            @pl.when(j2 > j)
            def _():
                reduce(j2, k, 0, to).start()

        @pl.when((k == 1) | (k == 2))
        def _():
            up, dn = place(1, 0, 0, 0), place(3, 0, 0, 0)
            reduce(j, k, 1, up).start()
            reduce(j, k, 3, dn).start()

            @pl.when(j2 > j)
            def _():
                reduce(j2, k, 1, up).start()
                reduce(j2, k, 3, dn).start()

    def reduce(j, k, dx, to):
        if dx == 0:
            src, dst = rss.at[j, k], rsr.at[j, 2]
        else:
            src = rss.at[j, k, pl.ds(192 * (dx // 2), 192)]
            dst = rsr.at[j, 4 - dx, pl.ds((k - 1) * 192, 192)]
        return pltpu.make_async_remote_copy(
            src_ref=src, dst_ref=dst, send_sem=sum_ssem, recv_sem=sum_rsem.at[j],
            device_id=to, device_id_type=MESH,
        )

    def small1():
        def partial(t, carry):
            part = jnp.dot(half, jnp.concatenate([wn[2 * t], wn[2 * t + 1]], axis=1), preferred_element_type=F32)
            for i in range(2):
                pall[2 * t + i] = part[0:1, i * TB : (i + 1) * TB]
            return carry

        lax.fori_loop(0, 24, partial, 0, unroll=6)
        for dy in range(4):
            for xx in range(4):
                for i in range(3):
                    t = tile_map[xx * 12 + (y + dy) % 4 * 3 + i]
                    psend[dy, xx, i : i + 1] = pall[t]
        o_in, o_out = (("o1", lambda: obs_all.at[r, pl.ds(0, 7)]),) * 2
        for dz, dc in line:
            send(obs_all.at[r, q], obs_all.at[r, q], dev(dz=dz, dc=dc), o_in, o_out)
        pbuf[y] = psend[0]
        p_in, p_out = ("p1", lambda: pbuf.at[pl.ds(0, 3)]), ("p1", lambda: psend.at[pl.ds(1, 3)])
        for d in (1, 2, 3):
            send(psend.at[d], pbuf.at[y], dev(dy=d), p_in, p_out)

    def small2():
        wait(got, "o1")
        wait(got, "p1")
        o_in, o_out = (("o2", lambda: obs_all.at[pl.ds(0, 3)]),) * 2
        for d in (1, 2, 3):
            send(obs_all.at[r], obs_all.at[r], dev(dy=d), o_in, o_out)
        tot[...] = (pbuf[0] + pbuf[1]) + (pbuf[2] + pbuf[3])
        tbuf[x] = tot[x]
        p_in, p_out = ("p2", lambda: tbuf.at[pl.ds(0, 3)]), ("p2", lambda: tot.at[pl.ds(0, 3)])
        for d in (1, 2, 3):
            send(tot.at[x_of[d]], tbuf.at[x], dev(dx=d), p_in, p_out)

    def small3():
        wait(got, "o2")
        wait(got, "p2")
        o_in, o_out = (("o3", lambda: obs_all.at[pl.ds(0, 12)]),) * 2
        for d in (1, 2, 3):
            send(obs_all.at[x_rows], obs_all.at[x_rows], dev(dx=d), o_in, o_out)
        qbuf[q] = (tbuf[0] + tbuf[1]) + (tbuf[2] + tbuf[3])
        p_in, p_out = (("p3", lambda: qbuf.at[pl.ds(0, 7)]),) * 2
        for dz, dc in line:
            send(qbuf.at[q], qbuf.at[q], dev(dz=dz, dc=dc), p_in, p_out)

    def small4():
        wait(got, "o3")
        wait(got, "p3")
        total = qbuf[0]
        for i in range(1, 8):
            total = total + qbuf[i]
        rhs[...] = total
        every = obs_all[...].reshape(16 * 8, 1, TB)
        block_of = lax.broadcasted_iota(jnp.int32, every.shape, 0)
        bal[...] = jnp.sum(jnp.where(block_of == plan[...], every, 0.0), axis=0)

    first_r = [(dy, i) for dy in (1, 2, 3, 0) for i in range(3)]
    for n in range(0, 12, 2):
        pair = first_r[n : n + 2]
        white = slot_pair(*[(x + R_CH[0][0][0]) % 4 * 12 + (y + dy) % 4 * 3 + i for dy, i in pair])
        flipped = white.T.astype(BF16)
        for m, (dy, i) in enumerate(pair):
            tile, rows = flipped[m * TB : (m + 1) * TB], pl.ds(i * TB, TB)
            if dy == 0:
                rbuf[0, 0, 0, 0, rows] = tile
            else:
                rsend[0, dy - 1, rows] = tile
    pl.semaphore_wait(barrier, len(places))
    spread_r(0)
    for dz, dc in line + [(0, 0)]:
        base = ((z + dz) % 4 * 2 + (c + dc) % 2) * 6
        white = slot_pair(base, base + 1).astype(BF16)
        for j in range(2):
            tile = white[:, j * TB : (j + 1) * TB]
            if (dz, dc) == (0, 0):
                cbuf[j, 0, 0] = tile
            else:
                csend[j, dz * 2 + dc - 1] = tile
    spread_c(0)
    lax.fori_loop(0, 24, whiten_pair, 0, unroll=6)
    stage_r(1)
    stage_c(1)
    spread_r(1)
    spread_c(1)
    stage_r(2)
    stage_c(2)
    stage_r(3)
    stage_c(3)
    r1(0)
    spread_r(2)
    c1(0)
    small1()
    r2(0)
    r1(1)
    c2(0)
    spread_c(2)
    c1(1)
    rd(0)
    re(0)
    r2(1)
    r1(2)
    spread_c(3)
    spread_r(3)
    small2()
    rf(0)
    cf(0)
    c2(1)

    def before1():
        rd(1)
        re(1)
        c1(2)
        r2(2)
        r1(3)
        rf(1)

    def before2():
        cf(1)

    def before4():
        c2(2)
        c1(3)
        rd(2)
        re(2)
        rf(2)

    def before6():
        r2(3)
        cf(2)

    def before8():
        c2(3)
        rd(3)

    def before9():
        small3()
        re(3)
        cf(3)

    def before12():
        rf(3)

    acts = (
        (1, before1), (2, before2), (4, before4), (6, before6), (8, before8), (9, before9), (12, before12),
    )

    def slot(s, carry):
        for i, act in acts:
            pl.when(s == i)(act)
        block(s)
        return carry

    lax.fori_loop(0, len(ORDER), slot, 0)
    small4()
    for j in range(NJ):
        arrived = rsr.at[j, pl.ds(1, 3)]
        pltpu.make_async_copy(arrived, arrived, sum_rsem.at[j]).wait()
        total = own[j]
        for dx in (1, 2, 3):
            total = total + rsr[j, dx].astype(F32)
        gram[:, j * TB : (j + 1) * TB] = total
    for name in left:
        wait(left, name)
    sent = rss.at[:, pl.ds(0, 3)]
    pltpu.make_async_copy(sent, sent, sum_ssem).wait()


def hand_over(gram, rhs, bal, gram_out, rhs_out, bal_out, flat, sem):
    for i in range(3):
        flat[i * TB : (i + 1) * TB] = rhs[i]
    pairs = ((gram, gram_out), (bal, bal_out), (flat, rhs_out))
    copies = [pltpu.make_async_copy(src, dst, sem.at[i]) for i, (src, dst) in enumerate(pairs)]
    for cp in copies:
        cp.start()
    for cp in copies:
        cp.wait()


def on_device(
    design, observations, gaps, noise_var, arc_lengths, arc_amp, arc_decay, plan, tile_map
):
    smem = pl.BlockSpec(memory_space=pltpu.SMEM)
    vmem = pl.BlockSpec(memory_space=pltpu.VMEM)
    gram, rhs, bal = pl.pallas_call(
        kernel,
        name="normal_equations",
        out_shape=(
            pltpu.VMEM((384, 768), F32),
            pltpu.VMEM((3, TB), F32),
            pltpu.VMEM((1, TB), F32),
        ),
        in_specs=[smem] * 4 + [vmem, pl.BlockSpec(memory_space=pl.ANY)] + [vmem] * 3,
        out_specs=(vmem, vmem, vmem),
        scratch_shapes=[
            pltpu.VMEM((48, TB, TB), BF16),
            pltpu.VMEM((48, TB, TB), BF16),
            pltpu.VMEM((48, TB, TB), BF16),
            pltpu.VMEM((48, 1, TB), F32),
            pltpu.VMEM((NA, 4, 2, 4, 384, TB), BF16),
            pltpu.VMEM((NA, 3, 384, TB), BF16),
            pltpu.VMEM((NJ, 4, 8, TB, TB), BF16),
            pltpu.VMEM((NJ, 7, TB, TB), BF16),
            pltpu.VMEM((NJ + 1, 384, TB), F32),
            pltpu.VMEM((NJ, 4, 384, TB), BF16),
            pltpu.VMEM((NJ, 4, 384, TB), BF16),
            pltpu.VMEM((16, 8, 1, TB), F32),
            pltpu.VMEM((4, 4, 3, TB), F32),
            pltpu.VMEM((4, 4, 3, TB), F32),
            pltpu.VMEM((8, 3, TB), F32),
            pltpu.VMEM((4, 3, TB), F32),
            pltpu.VMEM((4, 3, TB), F32),
            pltpu.SemaphoreType.DMA,
            pltpu.SemaphoreType.DMA((N_LEFT,)),
            pltpu.SemaphoreType.DMA((N_GOT,)),
            pltpu.SemaphoreType.DMA,
            pltpu.SemaphoreType.DMA((NJ,)),
        ],
        compiler_params=pltpu.CompilerParams(
            collective_id=0, has_side_effects=True, vmem_limit_bytes=60 * 1024 * 1024
        ),
    )(
        tile_map,
        arc_lengths,
        arc_amp,
        arc_decay,
        plan.reshape(1, 1),
        design,
        observations.reshape(1, TB),
        gaps.reshape(1, TB),
        noise_var.reshape(1, TB),
    )
    inner = [pltpu.with_memory_space_constraint(v, pltpu.VMEM) for v in (gram, rhs, bal)]
    anywhere = pl.BlockSpec(memory_space=pl.ANY)
    return pl.pallas_call(
        hand_over,
        name="hand_over",
        out_shape=(
            jax.ShapeDtypeStruct((384, 768), F32),
            jax.ShapeDtypeStruct((384,), F32),
            jax.ShapeDtypeStruct((1, TB), F32),
        ),
        in_specs=[vmem] * 3,
        out_specs=(anywhere, anywhere, anywhere),
        scratch_shapes=[pltpu.VMEM((384,), F32), pltpu.SemaphoreType.DMA((3,))],
        compiler_params=pltpu.CompilerParams(vmem_limit_bytes=1024 * 1024),
    )(*inner)


def solution(mesh):
    placed = (
        P(("row", "col"), None),
        P(("row", "col")),
        P(("row", "col")),
        P(("row", "col")),
        P(("row", "col"), None),
        P(("row", "col"), None),
        P(("row", "col"), None),
        P(("row", "col")),
        P(),
    )
    return jax.shard_map(
        on_device,
        mesh=mesh,
        in_specs=placed,
        out_specs=(P("row", "col"), P("row"), P(("row", "col"), None)),
        check_vma=False,
    )
```

```python
import jax
import jax.numpy as jnp
from jax import lax
from jax.experimental import pallas as pl
from jax.experimental.pallas import tpu as pltpu
from jax.sharding import PartitionSpec as P

MESH = pl.DeviceIdType.MESH
F32 = jnp.float32
BF16 = jnp.bfloat16
TB = 128
R_CH = (((2, 0, 384),), ((1, 0, 192), (3, 0, 192)), ((1, 192, 192), (3, 192, 192)), ((0, 0, 384),))
C_CH = ((0, 2), (2, 2), (4, 1), (5, 1))
NA, NB, NJ = len(R_CH), len(C_CH), 6
ORDER = (
    (0, 0, 1), (1, 0, 1), (0, 2, 3), (1, 2, 3), (2, 0, 1), (2, 2, 3), (0, 4, 4), (1, 4, 4), (2, 4, 4),
    (0, 5, 5), (1, 5, 5), (2, 5, 5), (3, 0, 1), (3, 2, 3), (3, 4, 5),
)
N_GOT, N_LEFT = 50, 13


def inverse_factor(lens, amps, decays, gaps, noise, obs):
    shape = (8, TB)
    pos = lax.broadcasted_iota(jnp.int32, shape, 1)
    live = jnp.broadcast_to(gaps, shape).astype(F32)
    noise = jnp.broadcast_to(noise, shape)
    e0 = lens[0, 0]
    e1 = e0 + lens[0, 1]
    e2 = e1 + lens[0, 2]

    def by_arc(p, v):
        return jnp.where(p < e0, v[0], jnp.where(p < e1, v[1], jnp.where(p < e2, v[2], v[3])))

    amp = by_arc(pos, [amps[0, i] for i in range(4)])
    decay = by_arc(pos, [decays[0, i] for i in range(4)])
    start = (pos == 0) | (pos == e0) | (pos == e1) | (pos == e2)
    gain = decay * decay
    q = amp * (1.0 - gain)
    live_prev = pltpu.roll(live, 1, 1) > 0.5
    noise_prev = pltpu.roll(noise, 1, 1)
    a = jnp.where(start, 0.0, jnp.where(live_prev, gain * noise_prev + q, gain))
    b = jnp.where(start, amp, jnp.where(live_prev, q * noise_prev, q))
    c = jnp.where(start, 0.0, jnp.where(live_prev, 1.0, 0.0))
    d = jnp.where(start, 1.0, jnp.where(live_prev, noise_prev, 1.0))
    for shift in (1, 2, 4, 8, 16, 32):
        ok = pos >= shift
        ap, bp = pltpu.roll(a, shift, 1), pltpu.roll(b, shift, 1)
        cp, dp = pltpu.roll(c, shift, 1), pltpu.roll(d, shift, 1)
        an = jnp.where(ok, a * ap + b * cp, a)
        bn = jnp.where(ok, a * bp + b * dp, b)
        cn = jnp.where(ok, c * ap + d * cp, c)
        dn = jnp.where(ok, c * bp + d * dp, d)
        if shift == 8:
            scale = 1.0 / (an + bn + cn + dn)
            an, bn, cn, dn = an * scale, bn * scale, cn * scale, dn * scale
        a, b, c, d = an, bn, cn, dn
    var = b / d
    is_live = live > 0.5
    total = jnp.where(is_live, var, 0.0) + noise
    root = live * lax.rsqrt(total)
    log_step = jnp.log(jnp.where(is_live, decay * (noise / total), decay))
    push = jnp.where(is_live, decay * (var / total), 0.0)
    sq = (TB, TB)
    row = lax.broadcasted_iota(jnp.int32, sq, 0)
    col = lax.broadcasted_iota(jnp.int32, sq, 1)
    upto = (row <= col).astype(F32)
    cum = jnp.dot(log_step, upto, precision=lax.Precision.HIGHEST, preferred_element_type=F32)
    before = cum - log_step
    eye = row == col

    def as_column(v):
        return jnp.sum(jnp.where(eye, jnp.broadcast_to(v[0:1], sq), 0.0), axis=1, keepdims=True)

    def arc_of(p):
        return by_arc(p, [0, 1, 2, 3])

    inside = (row > col) & (arc_of(row) == arc_of(col))
    span = jnp.where(inside, as_column(before) - cum[0:1], -1e30)
    lower = jnp.where(eye, 1.0, -jnp.exp(span) * push[0:1])
    inv = as_column(root) * lower
    white_col = jnp.sum(inv * obs, axis=1, keepdims=True)
    white_row = jnp.sum(jnp.where(eye, white_col, 0.0), axis=0, keepdims=True)
    return inv, white_row


def kernel(
    tile_map, lens, amps, decays, plan, design, obs, gaps, noise,
    gram, rhs, bal,
    dbuf, wn, wt, pall, rbuf, rsend, cbuf, csend, own, rss, rsr, obs_all, psend, pbuf, qbuf, tot, tbuf,
    load_sem, ssem, rsem, sum_ssem, sum_rsem,
):
    r, q = lax.axis_index("row"), lax.axis_index("col")
    x, y, z, c = r // 4, r % 4, q // 2, q % 2

    def place(dx, dy, dz, dc):
        return ((x + dx) % 4 * 4 + (y + dy) % 4, (z + dz) % 4 * 2 + (c + dc) % 2)

    steps = [(i, 0, 0, 0) for i in (1, 2, 3)] + [(0, i, 0, 0) for i in (1, 2, 3)]
    steps = steps + [(0, 0, i, j) for i in range(4) for j in range(2) if (i, j) != (0, 0)]
    places = {step: place(*step) for step in steps}

    def dev(dx=0, dy=0, dz=0, dc=0):
        return places[dx, dy, dz, dc]

    y_of = [(y + d) % 4 for d in range(4)]
    x_rows = pl.ds(4 * x, 4)

    got, left = {}, {}

    def group(table, sems, name, region):
        if name not in table:
            table[name] = (len(table), sems, region)
        return table[name][0]

    def wait(table, name):
        i, sems, region = table[name]
        pltpu.make_async_copy(region(), region(), sems.at[i]).wait()

    def send(src, dst, to, arrival, leaving):
        pltpu.make_async_remote_copy(
            src_ref=src, dst_ref=dst, send_sem=ssem.at[group(left, ssem, *leaving)], recv_sem=rsem.at[group(got, rsem, *arrival)],
            device_id=to, device_id_type=MESH,
        ).start()

    for t in range(48):
        pltpu.make_async_copy(design.at[:, pl.ds(t * TB, TB)], dbuf.at[t], load_sem).start()
    line = [(dz, dc) for dz in range(4) for dc in range(2) if (dz, dc) != (0, 0)]
    barrier = pltpu.get_barrier_semaphore()
    for p in places.values():
        pl.semaphore_signal(barrier, inc=1, device_id=p, device_id_type=MESH)

    inv, white_row = inverse_factor(lens, amps, decays, gaps[...], noise[...], obs[...])
    hi = inv.astype(BF16)
    lo = (inv - hi.astype(F32)).astype(BF16)
    both = jnp.concatenate([hi, lo], axis=1)
    obs_all[r, q] = white_row
    half = jnp.broadcast_to(white_row, (8, TB)).astype(BF16)
    pltpu.make_async_copy(dbuf, dbuf, load_sem).wait()

    def whitened(cols):
        return jnp.dot(both, jnp.concatenate([cols, cols], axis=0), preferred_element_type=F32)

    def slot_pair(s, s2):
        cols = [dbuf[tile_map[i]] for i in (s, s2)]
        return whitened(jnp.concatenate(cols, axis=1))

    def whiten_pair(t, carry):
        white = whitened(jnp.concatenate([dbuf[2 * t], dbuf[2 * t + 1]], axis=1))
        kept = white.astype(BF16)
        flipped = white.T.astype(BF16)
        for i in range(2):
            wn[2 * t + i] = kept[:, i * TB : (i + 1) * TB]
            wt[2 * t + i] = flipped[i * TB : (i + 1) * TB]
        return carry


    def stage_r(k):
        for dy in range(4):
            at = 0
            for dx, first, count in R_CH[k]:
                for i in range(3):
                    lo, hi = max(first, i * TB), min(first + count, i * TB + TB)
                    if lo < hi:
                        t = tile_map[(x + dx) % 4 * 12 + (y + dy) % 4 * 3 + i]
                        tile = wt[t, pl.ds(lo - i * TB, hi - lo)]
                        if dy == 0:
                            rbuf[k, 0, 0, 0, pl.ds(at, hi - lo)] = tile
                        else:
                            rsend[k, dy - 1, pl.ds(at, hi - lo)] = tile
                        at += hi - lo

    def stage_c(b):
        first, count = C_CH[b]
        for dz in range(4):
            for dc in range(2):
                for j in range(first, first + count):
                    t = tile_map[((z + dz) % 4 * 2 + (c + dc) % 2) * 6 + j]
                    if (dz, dc) == (0, 0):
                        cbuf[j, 0, 0] = wn[t]
                    else:
                        csend[j, dz * 2 + dc - 1] = wn[t]

    partner = dev(dc=1)
    y_up, y_dn, z_up, z_dn = dev(dy=1), dev(dy=3), dev(dz=1), dev(dz=3)

    r_left, c_left = ("r", lambda: rsend), ("c", lambda: csend)
    r1_left, r2_left = ("r1", lambda: rbuf.at[0]), ("r2", lambda: rbuf.at[0, pl.ds(0, 2)])
    c1_left, c2_left = ("c1", lambda: cbuf.at[pl.ds(0, 3)]), ("c2", lambda: cbuf.at[pl.ds(0, 3), pl.ds(0, 2)])
    over_left = ("over", lambda: rbuf.at[pl.ds(0, 2)])

    def tiles(b):
        return pl.ds(*C_CH[b])

    def spread_r(k):
        arrival = (f"r{k}", lambda: rbuf.at[k, 0, 0, pl.ds(1, 3)])
        for d in (1, 3, 2):
            send(rsend.at[k, d - 1], rbuf.at[k, 0, 0, 4 - d], dev(dy=d), arrival, r_left)

    def spread_c(b):
        arrival = (f"c{b}", lambda: cbuf.at[tiles(b), 0, pl.ds(1, 7)])
        for dz, dc in line:
            src = csend.at[tiles(b), dz * 2 + dc - 1]
            send(src, cbuf.at[tiles(b), 0, (4 - dz) % 4 * 2 + dc], dev(dz=dz, dc=dc), arrival, c_left)

    def r_ref(k, rz, part):
        return rbuf.at[k, rz, 0, part]

    def c_ref(b, ry, part):
        return cbuf.at[tiles(b), ry, part]

    def pieces(part):
        return [pl.ds(i, 1) for i in range(part.start, part.start + part.size)]

    def gather1(ref, i, up, dn, halves, name, leaving):
        first, second = halves
        wait(got, f"{name}{i}")
        one, other = (f"{name}up{i}", lambda: ref(i, 3, first)), (f"{name}dn{i}", lambda: ref(i, 1, second))
        rest = (f"{name}rest{i}", lambda: ref(i, 1, pl.ds(0, 2 * first.size)))
        for p, p2 in zip(pieces(first), pieces(second)):
            send(ref(i, 0, p), ref(i, 3, p), up, one, leaving)
            send(ref(i, 0, p2), ref(i, 1, p2), dn, other, leaving)
        send(ref(i, 0, second), ref(i, 3, second), up, rest, leaving)
        send(ref(i, 0, first), ref(i, 1, first), dn, rest, leaving)

    def gather2(ref, i, up, dn, halves, name, leaving):
        first, second = halves
        far = (f"{name}far{i}", lambda: ref(i, 2, pl.ds(0, 2 * first.size)))
        wait(got, f"{name}up{i}")
        for p in pieces(first):
            send(ref(i, 3, p), ref(i, 2, p), up, far, leaving)
        wait(got, f"{name}dn{i}")
        for p in pieces(second):
            send(ref(i, 1, p), ref(i, 2, p), dn, far, leaving)

    r_halves = (pl.ds(0, 2), pl.ds(2, 2))
    c_halves = (pl.ds(0, 4), pl.ds(4, 4))

    def over(k, rz):
        send(rbuf.at[k, rz, 0], rbuf.at[k, rz, 1], partner, (f"over{k}", lambda: rbuf.at[k, :, 1]), over_left)

    def r1(k):
        gather1(r_ref, k, z_up, z_dn, r_halves, "r", r1_left)
        over(k, 0)

    def r2(k):
        gather2(r_ref, k, z_up, z_dn, r_halves, "r", r2_left)

    def rd(k):
        wait(got, f"rrest{k}")
        over(k, 3)
        over(k, 1)

    def re(k):
        wait(got, f"rfar{k}")
        over(k, 2)

    def rf(k):
        wait(got, f"over{k}")

    def c1(b):
        gather1(c_ref, b, y_up, y_dn, c_halves, "c", c1_left)

    def c2(b):
        gather2(c_ref, b, y_up, y_dn, c_halves, "c", c2_left)

    def cf(b):
        wait(got, f"crest{b}")
        wait(got, f"cfar{b}")

    def pick(s, values):
        out = values[0]
        for i in range(1, len(values)):
            out = jnp.where(s == i, values[i], out)
        return out

    def block(s):
        k, j, j2 = (pick(s, [block[i] for block in ORDER]) for i in range(3))
        groups = [(rz, rc, ry) for rz in range(4) for rc in range(2) for ry in range(4)]
        lhs = jnp.concatenate([rbuf[k, rz, rc, ry] for rz, rc, ry in groups], axis=1)
        left = jnp.concatenate([cbuf[j, ry, rz * 2 + rc] for rz, rc, ry in groups], axis=0)
        right = jnp.concatenate([cbuf[j2, ry, rz * 2 + rc] for rz, rc, ry in groups], axis=0)
        value = jnp.dot(lhs, jnp.concatenate([left, right], axis=1), preferred_element_type=F32)
        last = k == NA - 1
        own[jnp.where(last, j, NJ)] = value[:, :TB]
        own[jnp.where(last, j2, NJ)] = value[:, TB:]
        rss[j, k] = value[:, :TB].astype(BF16)
        rss[j2, k] = value[:, TB:].astype(BF16)

        @pl.when(k == 0)
        def _():
            to = place(2, 0, 0, 0)
            reduce(j, k, 0, to).start()

            @pl.when(j2 > j)
            def _():
                reduce(j2, k, 0, to).start()

        @pl.when((k == 1) | (k == 2))
        def _():
            up, dn = place(1, 0, 0, 0), place(3, 0, 0, 0)
            reduce(j, k, 1, up).start()
            reduce(j, k, 3, dn).start()

            @pl.when(j2 > j)
            def _():
                reduce(j2, k, 1, up).start()
                reduce(j2, k, 3, dn).start()

    def reduce(j, k, dx, to):
        if dx == 0:
            src, dst = rss.at[j, k], rsr.at[j, 2]
        else:
            src = rss.at[j, k, pl.ds(192 * (dx // 2), 192)]
            dst = rsr.at[j, 4 - dx, pl.ds((k - 1) * 192, 192)]
        return pltpu.make_async_remote_copy(
            src_ref=src, dst_ref=dst, send_sem=sum_ssem, recv_sem=sum_rsem.at[j],
            device_id=to, device_id_type=MESH,
        )

    def small1():
        def partial(t, carry):
            part = jnp.dot(half, jnp.concatenate([wn[2 * t], wn[2 * t + 1]], axis=1), preferred_element_type=F32)
            for i in range(2):
                pall[2 * t + i] = part[0:1, i * TB : (i + 1) * TB]
            return carry

        lax.fori_loop(0, 24, partial, 0, unroll=6)
        for dx in range(4):
            for yy in range(4):
                for i in range(3):
                    t = tile_map[(x + dx) % 4 * 12 + yy * 3 + i]
                    psend[dx, yy, i : i + 1] = pall[t]
        o_in, o_out = (("o1", lambda: obs_all.at[r, pl.ds(0, 7)]),) * 2
        for dz, dc in line:
            send(obs_all.at[r, q], obs_all.at[r, q], dev(dz=dz, dc=dc), o_in, o_out)
        pbuf[x] = psend[0]
        p_in, p_out = ("p1", lambda: pbuf.at[pl.ds(0, 3)]), ("p1", lambda: psend.at[pl.ds(1, 3)])
        for d in (1, 2, 3):
            send(psend.at[d], pbuf.at[x], dev(dx=d), p_in, p_out)

    def small2():
        wait(got, "o1")
        wait(got, "p1")
        o_in, o_out = (("o2", lambda: obs_all.at[pl.ds(0, 3)]),) * 2
        for d in (1, 2, 3):
            send(obs_all.at[r], obs_all.at[r], dev(dy=d), o_in, o_out)
        tot[...] = (pbuf[0] + pbuf[1]) + (pbuf[2] + pbuf[3])
        tbuf[y] = tot[y]
        p_in, p_out = ("p2", lambda: tbuf.at[pl.ds(0, 3)]), ("p2", lambda: tot.at[pl.ds(0, 3)])
        for d in (1, 2, 3):
            send(tot.at[y_of[d]], tbuf.at[y], dev(dy=d), p_in, p_out)

    def small3():
        wait(got, "o2")
        wait(got, "p2")
        o_in, o_out = (("o3", lambda: obs_all.at[pl.ds(0, 12)]),) * 2
        for d in (1, 2, 3):
            send(obs_all.at[x_rows], obs_all.at[x_rows], dev(dx=d), o_in, o_out)
        qbuf[q] = (tbuf[0] + tbuf[1]) + (tbuf[2] + tbuf[3])
        p_in, p_out = (("p3", lambda: qbuf.at[pl.ds(0, 7)]),) * 2
        for dz, dc in line:
            send(qbuf.at[q], qbuf.at[q], dev(dz=dz, dc=dc), p_in, p_out)

    def small4():
        wait(got, "o3")
        wait(got, "p3")
        total = qbuf[0]
        for i in range(1, 8):
            total = total + qbuf[i]
        rhs[...] = total
        every = obs_all[...].reshape(16 * 8, 1, TB)
        block_of = lax.broadcasted_iota(jnp.int32, every.shape, 0)
        bal[...] = jnp.sum(jnp.where(block_of == plan[...], every, 0.0), axis=0)

    first_r = [(dy, i) for dy in (1, 2, 3, 0) for i in range(3)]
    for n in range(0, 12, 2):
        pair = first_r[n : n + 2]
        white = slot_pair(*[(x + R_CH[0][0][0]) % 4 * 12 + (y + dy) % 4 * 3 + i for dy, i in pair])
        flipped = white.T.astype(BF16)
        for m, (dy, i) in enumerate(pair):
            tile, rows = flipped[m * TB : (m + 1) * TB], pl.ds(i * TB, TB)
            if dy == 0:
                rbuf[0, 0, 0, 0, rows] = tile
            else:
                rsend[0, dy - 1, rows] = tile
    pl.semaphore_wait(barrier, len(places))
    spread_r(0)
    for dz, dc in line + [(0, 0)]:
        base = ((z + dz) % 4 * 2 + (c + dc) % 2) * 6
        white = slot_pair(base, base + 1).astype(BF16)
        for j in range(2):
            tile = white[:, j * TB : (j + 1) * TB]
            if (dz, dc) == (0, 0):
                cbuf[j, 0, 0] = tile
            else:
                csend[j, dz * 2 + dc - 1] = tile
    spread_c(0)
    lax.fori_loop(0, 24, whiten_pair, 0, unroll=6)
    stage_r(1)
    stage_c(1)
    spread_r(1)
    spread_c(1)
    stage_r(2)
    stage_c(2)
    stage_r(3)
    stage_c(3)
    spread_r(2)
    r1(0)
    c1(0)
    small1()
    r2(0)
    r1(1)
    c2(0)
    spread_c(2)
    c1(1)
    rd(0)
    re(0)
    r2(1)
    r1(2)
    spread_c(3)
    spread_r(3)
    small2()
    rf(0)
    cf(0)
    c2(1)

    def before1():
        rd(1)
        re(1)
        c1(2)
        r2(2)
        r1(3)
        rf(1)

    def before2():
        cf(1)

    def before4():
        c2(2)
        c1(3)
        rd(2)
        re(2)
        rf(2)

    def before6():
        r2(3)
        cf(2)

    def before8():
        c2(3)
        rd(3)

    def before9():
        small3()
        re(3)
        cf(3)

    def before12():
        rf(3)

    acts = (
        (1, before1), (2, before2), (4, before4), (6, before6), (8, before8), (9, before9), (12, before12),
    )

    def slot(s, carry):
        for i, act in acts:
            pl.when(s == i)(act)
        block(s)
        return carry

    lax.fori_loop(0, len(ORDER), slot, 0)
    small4()
    for j in range(NJ):
        arrived = rsr.at[j, pl.ds(1, 3)]
        pltpu.make_async_copy(arrived, arrived, sum_rsem.at[j]).wait()
        total = own[j]
        for dx in (1, 2, 3):
            total = total + rsr[j, dx].astype(F32)
        gram[:, j * TB : (j + 1) * TB] = total
    for name in left:
        wait(left, name)
    sent = rss.at[:, pl.ds(0, 3)]
    pltpu.make_async_copy(sent, sent, sum_ssem).wait()


def hand_over(gram, rhs, bal, gram_out, rhs_out, bal_out, flat, sem):
    for i in range(3):
        flat[i * TB : (i + 1) * TB] = rhs[i]
    rows = [pl.ds(i * 96, 96) for i in range(4)]
    pairs = [(gram.at[part], gram_out.at[part]) for part in rows] + [(bal, bal_out), (flat, rhs_out)]
    copies = [pltpu.make_async_copy(src, dst, sem.at[i]) for i, (src, dst) in enumerate(pairs)]
    for cp in copies:
        cp.start()
    for cp in copies:
        cp.wait()


def on_device(
    design, observations, gaps, noise_var, arc_lengths, arc_amp, arc_decay, plan, tile_map
):
    smem = pl.BlockSpec(memory_space=pltpu.SMEM)
    vmem = pl.BlockSpec(memory_space=pltpu.VMEM)
    gram, rhs, bal = pl.pallas_call(
        kernel,
        name="normal_equations",
        out_shape=(
            pltpu.VMEM((384, 768), F32),
            pltpu.VMEM((3, TB), F32),
            pltpu.VMEM((1, TB), F32),
        ),
        in_specs=[smem] * 4 + [vmem, pl.BlockSpec(memory_space=pl.ANY)] + [vmem] * 3,
        out_specs=(vmem, vmem, vmem),
        scratch_shapes=[
            pltpu.VMEM((48, TB, TB), BF16),
            pltpu.VMEM((48, TB, TB), BF16),
            pltpu.VMEM((48, TB, TB), BF16),
            pltpu.VMEM((48, 1, TB), F32),
            pltpu.VMEM((NA, 4, 2, 4, 384, TB), BF16),
            pltpu.VMEM((NA, 3, 384, TB), BF16),
            pltpu.VMEM((NJ, 4, 8, TB, TB), BF16),
            pltpu.VMEM((NJ, 7, TB, TB), BF16),
            pltpu.VMEM((NJ + 1, 384, TB), F32),
            pltpu.VMEM((NJ, 4, 384, TB), BF16),
            pltpu.VMEM((NJ, 4, 384, TB), BF16),
            pltpu.VMEM((16, 8, 1, TB), F32),
            pltpu.VMEM((4, 4, 3, TB), F32),
            pltpu.VMEM((4, 4, 3, TB), F32),
            pltpu.VMEM((8, 3, TB), F32),
            pltpu.VMEM((4, 3, TB), F32),
            pltpu.VMEM((4, 3, TB), F32),
            pltpu.SemaphoreType.DMA,
            pltpu.SemaphoreType.DMA((N_LEFT,)),
            pltpu.SemaphoreType.DMA((N_GOT,)),
            pltpu.SemaphoreType.DMA,
            pltpu.SemaphoreType.DMA((NJ,)),
        ],
        compiler_params=pltpu.CompilerParams(
            collective_id=0, has_side_effects=True, vmem_limit_bytes=60 * 1024 * 1024
        ),
    )(
        tile_map,
        arc_lengths,
        arc_amp,
        arc_decay,
        plan.reshape(1, 1),
        design,
        observations.reshape(1, TB),
        gaps.reshape(1, TB),
        noise_var.reshape(1, TB),
    )
    inner = [pltpu.with_memory_space_constraint(v, pltpu.VMEM) for v in (gram, rhs, bal)]
    anywhere = pl.BlockSpec(memory_space=pl.ANY)
    return pl.pallas_call(
        hand_over,
        name="hand_over",
        out_shape=(
            jax.ShapeDtypeStruct((384, 768), F32),
            jax.ShapeDtypeStruct((384,), F32),
            jax.ShapeDtypeStruct((1, TB), F32),
        ),
        in_specs=[vmem] * 3,
        out_specs=(anywhere, anywhere, anywhere),
        scratch_shapes=[pltpu.VMEM((384,), F32), pltpu.SemaphoreType.DMA((6,))],
        compiler_params=pltpu.CompilerParams(vmem_limit_bytes=1024 * 1024),
    )(*inner)


def solution(mesh):
    placed = (
        P(("row", "col"), None),
        P(("row", "col")),
        P(("row", "col")),
        P(("row", "col")),
        P(("row", "col"), None),
        P(("row", "col"), None),
        P(("row", "col"), None),
        P(("row", "col")),
        P(),
    )
    return jax.shard_map(
        on_device,
        mesh=mesh,
        in_specs=placed,
        out_specs=(P("row", "col"), P("row"), P(("row", "col"), None)),
        check_vma=False,
    )
```

```python
import jax
import jax.numpy as jnp
from jax import lax
from jax.experimental import pallas as pl
from jax.experimental.pallas import tpu as pltpu
from jax.sharding import PartitionSpec as P

MESH = pl.DeviceIdType.MESH
F32 = jnp.float32
BF16 = jnp.bfloat16
TB = 128
R_CH = (((2, 0, 384),), ((1, 0, 192), (3, 0, 192)), ((1, 192, 192), (3, 192, 192)), ((0, 0, 384),))
C_CH = ((0, 2), (2, 2), (4, 1), (5, 1))
NA, NB, NJ = len(R_CH), len(C_CH), 6
ORDER = (
    (0, 0, 1), (1, 0, 1), (0, 2, 3), (1, 2, 3), (2, 0, 1), (2, 2, 3), (0, 4, 4), (1, 4, 4), (2, 4, 4),
    (0, 5, 5), (1, 5, 5), (2, 5, 5), (3, 0, 1), (3, 2, 3), (3, 4, 5),
)
N_GOT, N_LEFT = 50, 13


def inverse_factor(lens, amps, decays, gaps, noise, obs):
    shape = (8, TB)
    pos = lax.broadcasted_iota(jnp.int32, shape, 1)
    live = jnp.broadcast_to(gaps, shape).astype(F32)
    noise = jnp.broadcast_to(noise, shape)
    e0 = lens[0, 0]
    e1 = e0 + lens[0, 1]
    e2 = e1 + lens[0, 2]

    def by_arc(p, v):
        return jnp.where(p < e0, v[0], jnp.where(p < e1, v[1], jnp.where(p < e2, v[2], v[3])))

    amp = by_arc(pos, [amps[0, i] for i in range(4)])
    decay = by_arc(pos, [decays[0, i] for i in range(4)])
    start = (pos == 0) | (pos == e0) | (pos == e1) | (pos == e2)
    gain = decay * decay
    q = amp * (1.0 - gain)
    live_prev = pltpu.roll(live, 1, 1) > 0.5
    noise_prev = pltpu.roll(noise, 1, 1)
    a = jnp.where(start, 0.0, jnp.where(live_prev, gain * noise_prev + q, gain))
    b = jnp.where(start, amp, jnp.where(live_prev, q * noise_prev, q))
    c = jnp.where(start, 0.0, jnp.where(live_prev, 1.0, 0.0))
    d = jnp.where(start, 1.0, jnp.where(live_prev, noise_prev, 1.0))
    for shift in (1, 4, 16):
        whole = (a, b, c, d)
        for n in (1, 2, 3):
            ok = pos >= n * shift
            ap, bp, cp, dp = (pltpu.roll(v, n * shift, 1) for v in whole)
            a, b, c, d = (
                jnp.where(ok, a * ap + b * cp, a),
                jnp.where(ok, a * bp + b * dp, b),
                jnp.where(ok, c * ap + d * cp, c),
                jnp.where(ok, c * bp + d * dp, d),
            )
        if shift == 4:
            scale = 1.0 / (a + b + c + d)
            a, b, c, d = a * scale, b * scale, c * scale, d * scale
    var = b / d
    is_live = live > 0.5
    total = jnp.where(is_live, var, 0.0) + noise
    root = live * lax.rsqrt(total)
    log_step = jnp.log(jnp.where(is_live, decay * (noise / total), decay))
    push = jnp.where(is_live, decay * (var / total), 0.0)
    sq = (TB, TB)
    row = lax.broadcasted_iota(jnp.int32, sq, 0)
    col = lax.broadcasted_iota(jnp.int32, sq, 1)
    upto = (row <= col).astype(F32)
    cum = jnp.dot(log_step, upto, precision=lax.Precision.HIGHEST, preferred_element_type=F32)
    before = cum - log_step
    eye = row == col

    def as_column(v):
        return jnp.sum(jnp.where(eye, jnp.broadcast_to(v[0:1], sq), 0.0), axis=1, keepdims=True)

    def arc_of(p):
        return by_arc(p, [0, 1, 2, 3])

    inside = (row > col) & (arc_of(row) == arc_of(col))
    span = jnp.where(inside, as_column(before) - cum[0:1], -1e30)
    lower = jnp.where(eye, 1.0, -jnp.exp(span) * push[0:1])
    inv = as_column(root) * lower
    white_col = jnp.sum(inv * obs, axis=1, keepdims=True)
    white_row = jnp.sum(jnp.where(eye, white_col, 0.0), axis=0, keepdims=True)
    return inv, white_row


def kernel(
    tile_map_in, lens_in, amps_in, decays_in, plan_in, design, obs_in, gaps_in, noise_in,
    gram, rhs, bal,
    tile_map, lens, amps, decays, plan, obs, gaps, noise, dbuf, wn, wt, pall, rbuf, rsend, cbuf, csend, own, rss, rsr, obs_all, psend, pbuf, qbuf, tot, tbuf,
    in_sem, load_sem, ssem, rsem, sum_ssem, sum_rsem,
):
    r, q = lax.axis_index("row"), lax.axis_index("col")
    x, y, z, c = r // 4, r % 4, q // 2, q % 2

    def place(dx, dy, dz, dc):
        return ((x + dx) % 4 * 4 + (y + dy) % 4, (z + dz) % 4 * 2 + (c + dc) % 2)

    steps = [(i, 0, 0, 0) for i in (1, 2, 3)] + [(0, i, 0, 0) for i in (1, 2, 3)]
    steps = steps + [(0, 0, i, j) for i in range(4) for j in range(2) if (i, j) != (0, 0)]
    places = {step: place(*step) for step in steps}

    def dev(dx=0, dy=0, dz=0, dc=0):
        return places[dx, dy, dz, dc]

    y_of = [(y + d) % 4 for d in range(4)]
    x_rows = pl.ds(4 * x, 4)

    got, left = {}, {}

    def group(table, sems, name, region):
        if name not in table:
            table[name] = (len(table), sems, region)
        return table[name][0]

    def wait(table, name):
        i, sems, region = table[name]
        pltpu.make_async_copy(region(), region(), sems.at[i]).wait()

    def send(src, dst, to, arrival, leaving):
        pltpu.make_async_remote_copy(
            src_ref=src, dst_ref=dst, send_sem=ssem.at[group(left, ssem, *leaving)], recv_sem=rsem.at[group(got, rsem, *arrival)],
            device_id=to, device_id_type=MESH,
        ).start()

    first = ((lens_in, lens), (amps_in, amps), (decays_in, decays), (gaps_in, gaps), (noise_in, noise), (obs_in, obs))
    pairs = first + ((tile_map_in, tile_map), (plan_in, plan))
    loads = [pltpu.make_async_copy(src, dst, in_sem.at[i]) for i, (src, dst) in enumerate(pairs)]
    for cp in loads:
        cp.start()
    for t in range(48):
        pltpu.make_async_copy(design.at[:, pl.ds(t * TB, TB)], dbuf.at[t], load_sem).start()
    line = [(dz, dc) for dz in range(4) for dc in range(2) if (dz, dc) != (0, 0)]
    barrier = pltpu.get_barrier_semaphore()
    for p in places.values():
        pl.semaphore_signal(barrier, inc=1, device_id=p, device_id_type=MESH)

    for cp in loads:
        cp.wait()
    inv, white_row = inverse_factor(lens, amps, decays, gaps[...], noise[...], obs[...])
    hi = inv.astype(BF16)
    lo = (inv - hi.astype(F32)).astype(BF16)
    both = jnp.concatenate([hi, lo], axis=1)
    obs_all[r, q] = white_row
    half = jnp.broadcast_to(white_row, (8, TB)).astype(BF16)
    pltpu.make_async_copy(dbuf, dbuf, load_sem).wait()

    def whitened(cols):
        return jnp.dot(both, jnp.concatenate([cols, cols], axis=0), preferred_element_type=F32)

    def slot_pair(s, s2):
        cols = [dbuf[tile_map[i]] for i in (s, s2)]
        return whitened(jnp.concatenate(cols, axis=1))

    def whiten_pair(t, carry):
        white = whitened(jnp.concatenate([dbuf[2 * t], dbuf[2 * t + 1]], axis=1))
        kept = white.astype(BF16)
        flipped = white.T.astype(BF16)
        for i in range(2):
            wn[2 * t + i] = kept[:, i * TB : (i + 1) * TB]
            wt[2 * t + i] = flipped[i * TB : (i + 1) * TB]
        return carry


    def stage_r(k):
        for dy in range(4):
            at = 0
            for dx, first, count in R_CH[k]:
                for i in range(3):
                    lo, hi = max(first, i * TB), min(first + count, i * TB + TB)
                    if lo < hi:
                        t = tile_map[(x + dx) % 4 * 12 + (y + dy) % 4 * 3 + i]
                        tile = wt[t, pl.ds(lo - i * TB, hi - lo)]
                        if dy == 0:
                            rbuf[k, 0, 0, 0, pl.ds(at, hi - lo)] = tile
                        else:
                            rsend[k, dy - 1, pl.ds(at, hi - lo)] = tile
                        at += hi - lo

    def stage_c(b):
        first, count = C_CH[b]
        for dz in range(4):
            for dc in range(2):
                for j in range(first, first + count):
                    t = tile_map[((z + dz) % 4 * 2 + (c + dc) % 2) * 6 + j]
                    if (dz, dc) == (0, 0):
                        cbuf[j, 0, 0] = wn[t]
                    else:
                        csend[j, dz * 2 + dc - 1] = wn[t]

    partner = dev(dc=1)
    y_up, y_dn, z_up, z_dn = dev(dy=1), dev(dy=3), dev(dz=1), dev(dz=3)

    r_left, c_left = ("r", lambda: rsend), ("c", lambda: csend)
    r1_left, r2_left = ("r1", lambda: rbuf.at[0]), ("r2", lambda: rbuf.at[0, pl.ds(0, 2)])
    c1_left, c2_left = ("c1", lambda: cbuf.at[pl.ds(0, 3)]), ("c2", lambda: cbuf.at[pl.ds(0, 3), pl.ds(0, 2)])
    over_left = ("over", lambda: rbuf.at[pl.ds(0, 2)])

    def tiles(b):
        return pl.ds(*C_CH[b])

    def spread_r(k):
        arrival = (f"r{k}", lambda: rbuf.at[k, 0, 0, pl.ds(1, 3)])
        for d in (1, 3, 2):
            send(rsend.at[k, d - 1], rbuf.at[k, 0, 0, 4 - d], dev(dy=d), arrival, r_left)

    def spread_c(b):
        arrival = (f"c{b}", lambda: cbuf.at[tiles(b), 0, pl.ds(1, 7)])
        for dz, dc in line:
            src = csend.at[tiles(b), dz * 2 + dc - 1]
            send(src, cbuf.at[tiles(b), 0, (4 - dz) % 4 * 2 + dc], dev(dz=dz, dc=dc), arrival, c_left)

    def r_ref(k, rz, part):
        return rbuf.at[k, rz, 0, part]

    def c_ref(b, ry, part):
        return cbuf.at[tiles(b), ry, part]

    def pieces(part):
        return [pl.ds(i, 1) for i in range(part.start, part.start + part.size)]

    def gather1(ref, i, up, dn, halves, name, leaving):
        first, second = halves
        wait(got, f"{name}{i}")
        one, other = (f"{name}up{i}", lambda: ref(i, 3, first)), (f"{name}dn{i}", lambda: ref(i, 1, second))
        rest = (f"{name}rest{i}", lambda: ref(i, 1, pl.ds(0, 2 * first.size)))
        for p, p2 in zip(pieces(first), pieces(second)):
            send(ref(i, 0, p), ref(i, 3, p), up, one, leaving)
            send(ref(i, 0, p2), ref(i, 1, p2), dn, other, leaving)
        send(ref(i, 0, second), ref(i, 3, second), up, rest, leaving)
        send(ref(i, 0, first), ref(i, 1, first), dn, rest, leaving)

    def gather2(ref, i, up, dn, halves, name, leaving):
        first, second = halves
        far = (f"{name}far{i}", lambda: ref(i, 2, pl.ds(0, 2 * first.size)))
        wait(got, f"{name}up{i}")
        for p in pieces(first):
            send(ref(i, 3, p), ref(i, 2, p), up, far, leaving)
        wait(got, f"{name}dn{i}")
        for p in pieces(second):
            send(ref(i, 1, p), ref(i, 2, p), dn, far, leaving)

    r_halves = (pl.ds(0, 2), pl.ds(2, 2))
    c_halves = (pl.ds(0, 4), pl.ds(4, 4))

    def over(k, rz):
        send(rbuf.at[k, rz, 0], rbuf.at[k, rz, 1], partner, (f"over{k}", lambda: rbuf.at[k, :, 1]), over_left)

    def r1(k):
        gather1(r_ref, k, z_up, z_dn, r_halves, "r", r1_left)
        over(k, 0)

    def r2(k):
        gather2(r_ref, k, z_up, z_dn, r_halves, "r", r2_left)

    def rd(k):
        wait(got, f"rrest{k}")
        over(k, 3)
        over(k, 1)

    def re(k):
        wait(got, f"rfar{k}")
        over(k, 2)

    def rf(k):
        wait(got, f"over{k}")

    def c1(b):
        gather1(c_ref, b, y_up, y_dn, c_halves, "c", c1_left)

    def c2(b):
        gather2(c_ref, b, y_up, y_dn, c_halves, "c", c2_left)

    def cf(b):
        wait(got, f"crest{b}")
        wait(got, f"cfar{b}")

    def pick(s, values):
        out = values[0]
        for i in range(1, len(values)):
            out = jnp.where(s == i, values[i], out)
        return out

    def block(s):
        k, j, j2 = (pick(s, [block[i] for block in ORDER]) for i in range(3))
        groups = [(rz, rc, ry) for rz in range(4) for rc in range(2) for ry in range(4)]
        lhs = jnp.concatenate([rbuf[k, rz, rc, ry] for rz, rc, ry in groups], axis=1)
        early = (j == NJ - 1) & (j2 == NJ - 1)
        far, far2 = jnp.where(early, NJ, j), jnp.where(early, NJ, j2)
        left = jnp.concatenate([cbuf[far if ry == 2 else j, ry, rz * 2 + rc] for rz, rc, ry in groups], axis=0)
        right = jnp.concatenate([cbuf[far2 if ry == 2 else j2, ry, rz * 2 + rc] for rz, rc, ry in groups], axis=0)
        value = jnp.dot(lhs, jnp.concatenate([left, right], axis=1), preferred_element_type=F32)
        last = k == NA - 1
        own[jnp.where(last, j, jnp.where(early, NJ + 1 + k, NJ))] = value[:, :TB]
        own[jnp.where(last, j2, NJ)] = value[:, TB:]
        rss[j, k] = value[:, :TB].astype(BF16)
        rss[j2, k] = value[:, TB:].astype(BF16)

        pl.when(jnp.logical_not(early))(lambda: reduce_tile(j, k))
        pl.when(j2 > j)(lambda: reduce_tile(j2, k))

    def late(k, carry):
        lhs = jnp.concatenate([rbuf[k, rz, rc, 2] for rz in range(4) for rc in range(2)], axis=1)
        right = jnp.concatenate([cbuf[NJ - 1, 2, i] for i in range(8)], axis=0)
        value = own[NJ + 1 + k] + jnp.dot(lhs, right, preferred_element_type=F32)
        rss[NJ - 1, k] = value.astype(BF16)
        reduce_tile(NJ - 1, k)
        return carry

    def reduce_tile(j, k):
        @pl.when(k == 0)
        def _():
            reduce(j, k, 0, place(2, 0, 0, 0)).start()

        @pl.when((k == 1) | (k == 2))
        def _():
            reduce(j, k, 1, place(1, 0, 0, 0)).start()
            reduce(j, k, 3, place(3, 0, 0, 0)).start()

    def reduce(j, k, dx, to):
        if dx == 0:
            src, dst = rss.at[j, k], rsr.at[j, 2]
        else:
            src = rss.at[j, k, pl.ds(192 * (dx // 2), 192)]
            dst = rsr.at[j, 4 - dx, pl.ds((k - 1) * 192, 192)]
        return pltpu.make_async_remote_copy(
            src_ref=src, dst_ref=dst, send_sem=sum_ssem, recv_sem=sum_rsem.at[j],
            device_id=to, device_id_type=MESH,
        )

    def small1():
        def partial(t, carry):
            part = jnp.dot(half, jnp.concatenate([wn[2 * t], wn[2 * t + 1]], axis=1), preferred_element_type=F32)
            for i in range(2):
                pall[2 * t + i] = part[0:1, i * TB : (i + 1) * TB]
            return carry

        lax.fori_loop(0, 24, partial, 0, unroll=6)
        for dx in range(4):
            for yy in range(4):
                for i in range(3):
                    t = tile_map[(x + dx) % 4 * 12 + yy * 3 + i]
                    psend[dx, yy, i : i + 1] = pall[t]
        o_in, o_out = (("o1", lambda: obs_all.at[r, pl.ds(0, 7)]),) * 2
        for dz, dc in line:
            send(obs_all.at[r, q], obs_all.at[r, q], dev(dz=dz, dc=dc), o_in, o_out)
        pbuf[x] = psend[0]
        p_in, p_out = ("p1", lambda: pbuf.at[pl.ds(0, 3)]), ("p1", lambda: psend.at[pl.ds(1, 3)])
        for d in (1, 2, 3):
            send(psend.at[d], pbuf.at[x], dev(dx=d), p_in, p_out)

    def small2():
        wait(got, "o1")
        wait(got, "p1")
        o_in, o_out = (("o2", lambda: obs_all.at[pl.ds(0, 3)]),) * 2
        for d in (1, 2, 3):
            send(obs_all.at[r], obs_all.at[r], dev(dy=d), o_in, o_out)
        tot[...] = (pbuf[0] + pbuf[1]) + (pbuf[2] + pbuf[3])
        tbuf[y] = tot[y]
        p_in, p_out = ("p2", lambda: tbuf.at[pl.ds(0, 3)]), ("p2", lambda: tot.at[pl.ds(0, 3)])
        for d in (1, 2, 3):
            send(tot.at[y_of[d]], tbuf.at[y], dev(dy=d), p_in, p_out)

    def small3():
        wait(got, "o2")
        wait(got, "p2")
        o_in, o_out = (("o3", lambda: obs_all.at[pl.ds(0, 12)]),) * 2
        for d in (1, 2, 3):
            send(obs_all.at[x_rows], obs_all.at[x_rows], dev(dx=d), o_in, o_out)
        qbuf[q] = (tbuf[0] + tbuf[1]) + (tbuf[2] + tbuf[3])
        p_in, p_out = (("p3", lambda: qbuf.at[pl.ds(0, 7)]),) * 2
        for dz, dc in line:
            send(qbuf.at[q], qbuf.at[q], dev(dz=dz, dc=dc), p_in, p_out)

    def small4():
        wait(got, "o3")
        wait(got, "p3")
        total = qbuf[0]
        for i in range(1, 8):
            total = total + qbuf[i]
        rhs[...] = total
        every = obs_all[...].reshape(16 * 8, 1, TB)
        block_of = lax.broadcasted_iota(jnp.int32, every.shape, 0)
        bal[...] = jnp.sum(jnp.where(block_of == plan[...], every, 0.0), axis=0)

    first_r = [(dy, i) for dy in (1, 2, 3, 0) for i in range(3)]
    for n in range(0, 12, 2):
        pair = first_r[n : n + 2]
        white = slot_pair(*[(x + R_CH[0][0][0]) % 4 * 12 + (y + dy) % 4 * 3 + i for dy, i in pair])
        flipped = white.T.astype(BF16)
        for m, (dy, i) in enumerate(pair):
            tile, rows = flipped[m * TB : (m + 1) * TB], pl.ds(i * TB, TB)
            if dy == 0:
                rbuf[0, 0, 0, 0, rows] = tile
            else:
                rsend[0, dy - 1, rows] = tile
    pl.semaphore_wait(barrier, len(places))
    spread_r(0)
    for dz, dc in line + [(0, 0)]:
        base = ((z + dz) % 4 * 2 + (c + dc) % 2) * 6
        white = slot_pair(base, base + 1).astype(BF16)
        for j in range(2):
            tile = white[:, j * TB : (j + 1) * TB]
            if (dz, dc) == (0, 0):
                cbuf[j, 0, 0] = tile
            else:
                csend[j, dz * 2 + dc - 1] = tile
    spread_c(0)
    lax.fori_loop(0, 24, whiten_pair, 0, unroll=6)
    stage_r(1)
    stage_c(1)
    spread_r(1)
    spread_c(1)
    stage_r(2)
    stage_c(2)
    stage_r(3)
    stage_c(3)
    spread_r(2)
    cbuf[NJ, 2] = jnp.zeros((8, TB, TB), BF16)
    r1(0)
    c1(0)
    small1()
    r2(0)
    r1(1)
    c2(0)
    spread_c(2)
    c1(1)
    rd(0)
    re(0)
    r2(1)
    r1(2)
    spread_c(3)
    spread_r(3)
    small2()
    rf(0)
    cf(0)
    c2(1)

    def before1():
        rd(1)
        re(1)
        c1(2)
        r2(2)
        r1(3)
        rf(1)

    def before2():
        cf(1)

    def before4():
        c2(2)
        c1(3)
        rd(2)
        re(2)
        rf(2)

    def before6():
        r2(3)
        cf(2)

    def before8():
        c2(3)
        rd(3)

    def before9():
        small3()
        wait(got, "crest3")

    def before11():
        re(3)

    def before12():
        wait(got, "cfar3")
        lax.fori_loop(0, 3, late, 0)
        rf(3)

    acts = (
        (1, before1), (2, before2), (4, before4), (6, before6), (8, before8), (9, before9), (11, before11), (12, before12),
    )

    def slot(s, carry):
        for i, act in acts:
            pl.when(s == i)(act)
        block(s)
        return carry

    lax.fori_loop(0, len(ORDER), slot, 0)
    small4()
    for j in range(NJ):
        arrived = rsr.at[j, pl.ds(1, 3)]
        pltpu.make_async_copy(arrived, arrived, sum_rsem.at[j]).wait()
        total = own[j]
        for dx in (1, 2, 3):
            total = total + rsr[j, dx].astype(F32)
        gram[:, j * TB : (j + 1) * TB] = total
    for name in left:
        wait(left, name)
    sent = rss.at[:, pl.ds(0, 3)]
    pltpu.make_async_copy(sent, sent, sum_ssem).wait()


def hand_over(gram, rhs, bal, gram_out, rhs_out, bal_out, flat, sem):
    for i in range(3):
        flat[i * TB : (i + 1) * TB] = rhs[i]
    rows = [pl.ds(i * 96, 96) for i in range(4)]
    pairs = [(gram.at[part], gram_out.at[part]) for part in rows] + [(bal, bal_out), (flat, rhs_out)]
    copies = [pltpu.make_async_copy(src, dst, sem.at[i]) for i, (src, dst) in enumerate(pairs)]
    for cp in copies:
        cp.start()
    for cp in copies:
        cp.wait()


def on_device(
    design, observations, gaps, noise_var, arc_lengths, arc_amp, arc_decay, plan, tile_map
):
    vmem = pl.BlockSpec(memory_space=pltpu.VMEM)
    gram, rhs, bal = pl.pallas_call(
        kernel,
        name="normal_equations",
        out_shape=(
            pltpu.VMEM((384, 768), F32),
            pltpu.VMEM((3, TB), F32),
            pltpu.VMEM((1, TB), F32),
        ),
        in_specs=[pl.BlockSpec(memory_space=pl.ANY)] * 9,
        out_specs=(vmem, vmem, vmem),
        scratch_shapes=[
            pltpu.SMEM((48,), jnp.int32),
            pltpu.SMEM((1, 4), jnp.int32),
            pltpu.SMEM((1, 4), F32),
            pltpu.SMEM((1, 4), F32),
            pltpu.VMEM((1, 1), jnp.int32),
            pltpu.VMEM((1, TB), F32),
            pltpu.VMEM((1, TB), jnp.int32),
            pltpu.VMEM((1, TB), F32),
            pltpu.VMEM((48, TB, TB), BF16),
            pltpu.VMEM((48, TB, TB), BF16),
            pltpu.VMEM((48, TB, TB), BF16),
            pltpu.VMEM((48, 1, TB), F32),
            pltpu.VMEM((NA, 4, 2, 4, 384, TB), BF16),
            pltpu.VMEM((NA, 3, 384, TB), BF16),
            pltpu.VMEM((NJ + 1, 4, 8, TB, TB), BF16),
            pltpu.VMEM((NJ, 7, TB, TB), BF16),
            pltpu.VMEM((NJ + 4, 384, TB), F32),
            pltpu.VMEM((NJ, 4, 384, TB), BF16),
            pltpu.VMEM((NJ, 4, 384, TB), BF16),
            pltpu.VMEM((16, 8, 1, TB), F32),
            pltpu.VMEM((4, 4, 3, TB), F32),
            pltpu.VMEM((4, 4, 3, TB), F32),
            pltpu.VMEM((8, 3, TB), F32),
            pltpu.VMEM((4, 3, TB), F32),
            pltpu.VMEM((4, 3, TB), F32),
            pltpu.SemaphoreType.DMA((8,)),
            pltpu.SemaphoreType.DMA,
            pltpu.SemaphoreType.DMA((N_LEFT,)),
            pltpu.SemaphoreType.DMA((N_GOT,)),
            pltpu.SemaphoreType.DMA,
            pltpu.SemaphoreType.DMA((NJ,)),
        ],
        compiler_params=pltpu.CompilerParams(
            collective_id=0, has_side_effects=True, vmem_limit_bytes=60 * 1024 * 1024
        ),
    )(
        tile_map,
        arc_lengths,
        arc_amp,
        arc_decay,
        plan.reshape(1, 1),
        design,
        observations.reshape(1, TB),
        gaps.reshape(1, TB),
        noise_var.reshape(1, TB),
    )
    inner = [pltpu.with_memory_space_constraint(v, pltpu.VMEM) for v in (gram, rhs, bal)]
    anywhere = pl.BlockSpec(memory_space=pl.ANY)
    return pl.pallas_call(
        hand_over,
        name="hand_over",
        out_shape=(
            jax.ShapeDtypeStruct((384, 768), F32),
            jax.ShapeDtypeStruct((384,), F32),
            jax.ShapeDtypeStruct((1, TB), F32),
        ),
        in_specs=[vmem] * 3,
        out_specs=(anywhere, anywhere, anywhere),
        scratch_shapes=[pltpu.VMEM((384,), F32), pltpu.SemaphoreType.DMA((6,))],
        compiler_params=pltpu.CompilerParams(vmem_limit_bytes=1024 * 1024),
    )(*inner)


def solution(mesh):
    placed = (
        P(("row", "col"), None),
        P(("row", "col")),
        P(("row", "col")),
        P(("row", "col")),
        P(("row", "col"), None),
        P(("row", "col"), None),
        P(("row", "col"), None),
        P(("row", "col")),
        P(),
    )
    return jax.shard_map(
        on_device,
        mesh=mesh,
        in_specs=placed,
        out_specs=(P("row", "col"), P("row"), P(("row", "col"), None)),
        check_vma=False,
    )
```

```python
import jax
import jax.numpy as jnp
from jax import lax
from jax.experimental import pallas as pl
from jax.experimental.pallas import tpu as pltpu
from jax.sharding import PartitionSpec as P

MESH = pl.DeviceIdType.MESH
F32 = jnp.float32
BF16 = jnp.bfloat16
TB = 128
R_CH = (((2, 0, 384),), ((1, 0, 192), (3, 0, 192)), ((1, 192, 192), (3, 192, 192)), ((0, 0, 384),))
C_CH = ((0, 2), (2, 2), (4, 1), (5, 1))
NA, NB, NJ = len(R_CH), len(C_CH), 6
ORDER = (
    (0, 0, 1), (1, 0, 1), (0, 2, 3), (1, 2, 3), (2, 0, 1), (2, 2, 3), (0, 4, 4), (1, 4, 4), (2, 4, 4),
    (0, 5, 5), (1, 5, 5), (2, 5, 5), (3, 0, 1), (3, 2, 3), (3, 4, 5),
)
N_GOT, N_LEFT = 47, 13


def inverse_factor(lens, amps, decays, gaps, noise, obs):
    shape = (8, TB)
    pos = lax.broadcasted_iota(jnp.int32, shape, 1)
    live = jnp.broadcast_to(gaps, shape).astype(F32)
    noise = jnp.broadcast_to(noise, shape)
    e0 = lens[0, 0]
    e1 = e0 + lens[0, 1]
    e2 = e1 + lens[0, 2]

    def by_arc(p, v):
        return jnp.where(p < e0, v[0], jnp.where(p < e1, v[1], jnp.where(p < e2, v[2], v[3])))

    amp = by_arc(pos, [amps[0, i] for i in range(4)])
    decay = by_arc(pos, [decays[0, i] for i in range(4)])
    start = (pos == 0) | (pos == e0) | (pos == e1) | (pos == e2)
    gain = decay * decay
    q = amp * (1.0 - gain)
    live_prev = pltpu.roll(live, 1, 1) > 0.5
    noise_prev = pltpu.roll(noise, 1, 1)
    a = jnp.where(start, 0.0, jnp.where(live_prev, gain * noise_prev + q, gain))
    b = jnp.where(start, amp, jnp.where(live_prev, q * noise_prev, q))
    c = jnp.where(start, 0.0, jnp.where(live_prev, 1.0, 0.0))
    d = jnp.where(start, 1.0, jnp.where(live_prev, noise_prev, 1.0))
    for shift in (1, 4, 16):
        whole = (a, b, c, d)
        for n in (1, 2, 3):
            ok = pos >= n * shift
            ap, bp, cp, dp = (pltpu.roll(v, n * shift, 1) for v in whole)
            a, b, c, d = (
                jnp.where(ok, a * ap + b * cp, a),
                jnp.where(ok, a * bp + b * dp, b),
                jnp.where(ok, c * ap + d * cp, c),
                jnp.where(ok, c * bp + d * dp, d),
            )
        if shift == 4:
            scale = 1.0 / (a + b + c + d)
            a, b, c, d = a * scale, b * scale, c * scale, d * scale
    var = b / d
    is_live = live > 0.5
    total = jnp.where(is_live, var, 0.0) + noise
    root = live * lax.rsqrt(total)
    log_step = jnp.log(jnp.where(is_live, decay * (noise / total), decay))
    push = jnp.where(is_live, decay * (var / total), 0.0)
    sq = (TB, TB)
    row = lax.broadcasted_iota(jnp.int32, sq, 0)
    col = lax.broadcasted_iota(jnp.int32, sq, 1)
    upto = (row <= col).astype(F32)
    cum = jnp.dot(log_step, upto, precision=lax.Precision.HIGHEST, preferred_element_type=F32)
    before = cum - log_step
    eye = row == col

    def as_column(v):
        return jnp.sum(jnp.where(eye, jnp.broadcast_to(v[0:1], sq), 0.0), axis=1, keepdims=True)

    def arc_of(p):
        return by_arc(p, [0, 1, 2, 3])

    inside = (row > col) & (arc_of(row) == arc_of(col))
    span = jnp.where(inside, as_column(before) - cum[0:1], -1e30)
    lower = jnp.where(eye, 1.0, -jnp.exp(span) * push[0:1])
    inv = as_column(root) * lower
    white_col = jnp.sum(inv * obs, axis=1, keepdims=True)
    white_row = jnp.sum(jnp.where(eye, white_col, 0.0), axis=0, keepdims=True)
    return inv, white_row


def kernel(
    tile_map_in, lens_in, amps_in, decays_in, plan_in, design, obs_in, gaps_in, noise_in,
    gram, rhs, bal,
    tile_map, lens, amps, decays, plan, obs, gaps, noise, dbuf, wn, wt, pall, rbuf, rsend, cbuf, csend, own, rss, rsr, obs_all, psend, pbuf, qbuf, tot, tbuf,
    in_sem, load_sem, ssem, rsem, sum_ssem, sum_rsem,
):
    r, q = lax.axis_index("row"), lax.axis_index("col")
    x, y, z, c = r // 4, r % 4, q // 2, q % 2

    def place(dx, dy, dz, dc):
        return ((x + dx) % 4 * 4 + (y + dy) % 4, (z + dz) % 4 * 2 + (c + dc) % 2)

    steps = [(i, 0, 0, 0) for i in (1, 2, 3)] + [(0, i, 0, 0) for i in (1, 2, 3)]
    steps = steps + [(0, 0, i, j) for i in range(4) for j in range(2) if (i, j) != (0, 0)]
    places = {step: place(*step) for step in steps}

    def dev(dx=0, dy=0, dz=0, dc=0):
        return places[dx, dy, dz, dc]

    y_of = [(y + d) % 4 for d in range(4)]
    x_rows = pl.ds(4 * x, 4)

    got, left = {}, {}

    def group(table, sems, name, region):
        if name not in table:
            table[name] = (len(table), sems, region)
        return table[name][0]

    def wait(table, name):
        i, sems, region = table[name]
        pltpu.make_async_copy(region(), region(), sems.at[i]).wait()

    def send(src, dst, to, arrival, leaving):
        pltpu.make_async_remote_copy(
            src_ref=src, dst_ref=dst, send_sem=ssem.at[group(left, ssem, *leaving)], recv_sem=rsem.at[group(got, rsem, *arrival)],
            device_id=to, device_id_type=MESH,
        ).start()

    first = ((lens_in, lens), (amps_in, amps), (decays_in, decays), (gaps_in, gaps), (noise_in, noise), (obs_in, obs))
    pairs = first + ((tile_map_in, tile_map), (plan_in, plan))
    loads = [pltpu.make_async_copy(src, dst, in_sem.at[i]) for i, (src, dst) in enumerate(pairs)]
    for cp in loads:
        cp.start()
    for t in range(48):
        pltpu.make_async_copy(design.at[:, pl.ds(t * TB, TB)], dbuf.at[t], load_sem).start()
    line = [(dz, dc) for dz in range(4) for dc in range(2) if (dz, dc) != (0, 0)]
    barrier = pltpu.get_barrier_semaphore()
    for p in places.values():
        pl.semaphore_signal(barrier, inc=1, device_id=p, device_id_type=MESH)

    for cp in loads:
        cp.wait()
    inv, white_row = inverse_factor(lens, amps, decays, gaps[...], noise[...], obs[...])
    hi = inv.astype(BF16)
    lo = (inv - hi.astype(F32)).astype(BF16)
    both = jnp.concatenate([hi, lo], axis=1)
    obs_all[r, q] = white_row
    half = jnp.broadcast_to(white_row, (8, TB)).astype(BF16)
    pltpu.make_async_copy(dbuf, dbuf, load_sem).wait()

    def whitened(cols):
        return jnp.dot(both, jnp.concatenate([cols, cols], axis=0), preferred_element_type=F32)

    def slot_pair(s, s2):
        cols = [dbuf[tile_map[i]] for i in (s, s2)]
        return whitened(jnp.concatenate(cols, axis=1))

    def whiten_pair(t, carry):
        white = whitened(jnp.concatenate([dbuf[2 * t], dbuf[2 * t + 1]], axis=1))
        kept = white.astype(BF16)
        flipped = white.T.astype(BF16)
        for i in range(2):
            wn[2 * t + i] = kept[:, i * TB : (i + 1) * TB]
            wt[2 * t + i] = flipped[i * TB : (i + 1) * TB]
        return carry


    def stage_r(k):
        for dy in range(4):
            at = 0
            for dx, first, count in R_CH[k]:
                for i in range(3):
                    lo, hi = max(first, i * TB), min(first + count, i * TB + TB)
                    if lo < hi:
                        t = tile_map[(x + dx) % 4 * 12 + (y + dy) % 4 * 3 + i]
                        tile = wt[t, pl.ds(lo - i * TB, hi - lo)]
                        if dy == 0:
                            rbuf[k, 0, 0, 0, pl.ds(at, hi - lo)] = tile
                        else:
                            rsend[k, dy - 1, pl.ds(at, hi - lo)] = tile
                        at += hi - lo

    def stage_c(b):
        first, count = C_CH[b]
        for dz in range(4):
            for dc in range(2):
                for j in range(first, first + count):
                    t = tile_map[((z + dz) % 4 * 2 + (c + dc) % 2) * 6 + j]
                    if (dz, dc) == (0, 0):
                        cbuf[j, 0, 0] = wn[t]
                    else:
                        csend[j, dz * 2 + dc - 1] = wn[t]

    partner = dev(dc=1)
    y_up, y_dn, z_up, z_dn = dev(dy=1), dev(dy=3), dev(dz=1), dev(dz=3)

    r_left, c_left = ("r", lambda: rsend), ("c", lambda: csend)
    r1_left, r2_left = ("r1", lambda: rbuf.at[0]), ("r2", lambda: rbuf.at[0, pl.ds(0, 2)])
    c1_left, c2_left = ("c1", lambda: cbuf.at[pl.ds(0, 3)]), ("c2", lambda: cbuf.at[pl.ds(0, 3), pl.ds(0, 2)])
    over_left = ("over", lambda: rbuf.at[pl.ds(0, 2)])

    def tiles(b):
        return pl.ds(*C_CH[b])

    def spread_r(k):
        arrival = (f"r{k}", lambda: rbuf.at[k, 0, 0, pl.ds(1, 3)])
        for d in (1, 3, 2):
            send(rsend.at[k, d - 1], rbuf.at[k, 0, 0, 4 - d], dev(dy=d), arrival, r_left)

    def spread_c(b):
        arrival = (f"c{b}", lambda: cbuf.at[tiles(b), 0, pl.ds(1, 7)])
        for dz, dc in line:
            src = csend.at[tiles(b), dz * 2 + dc - 1]
            send(src, cbuf.at[tiles(b), 0, (4 - dz) % 4 * 2 + dc], dev(dz=dz, dc=dc), arrival, c_left)

    def r_ref(k, rz, part):
        return rbuf.at[k, rz, 0, part]

    def c_ref(b, ry, part):
        return cbuf.at[tiles(b), ry, part]

    def pieces(part):
        return [pl.ds(i, 1) for i in range(part.start, part.start + part.size)]

    def c_both(b):
        return (f"cboth{b}", lambda: cbuf.at[tiles(b), pl.ds(1, 2)])

    def gather1(ref, i, up, dn, halves, name, leaving):
        first, second = halves
        wait(got, f"{name}{i}")
        one, other = (f"{name}up{i}", lambda: ref(i, 3, first)), (f"{name}dn{i}", lambda: ref(i, 1, second))
        rest = (f"{name}rest{i}", lambda: ref(i, 1, pl.ds(0, 2 * first.size)))
        if name == "c" and i < NB - 1:
            rest = c_both(i)
        for p, p2 in zip(pieces(first), pieces(second)):
            send(ref(i, 0, p), ref(i, 3, p), up, one, leaving)
            send(ref(i, 0, p2), ref(i, 1, p2), dn, other, leaving)
        send(ref(i, 0, second), ref(i, 3, second), up, rest, leaving)
        send(ref(i, 0, first), ref(i, 1, first), dn, rest, leaving)

    def gather2(ref, i, up, dn, halves, name, leaving):
        first, second = halves
        far = (f"{name}far{i}", lambda: ref(i, 2, pl.ds(0, 2 * first.size)))
        if name == "c" and i < NB - 1:
            far = c_both(i)
        wait(got, f"{name}up{i}")
        for p in pieces(first):
            send(ref(i, 3, p), ref(i, 2, p), up, far, leaving)
        wait(got, f"{name}dn{i}")
        for p in pieces(second):
            send(ref(i, 1, p), ref(i, 2, p), dn, far, leaving)

    r_halves = (pl.ds(0, 2), pl.ds(2, 2))
    c_halves = (pl.ds(0, 4), pl.ds(4, 4))

    def over(k, rz):
        send(rbuf.at[k, rz, 0], rbuf.at[k, rz, 1], partner, (f"over{k}", lambda: rbuf.at[k, :, 1]), over_left)

    def r1(k):
        gather1(r_ref, k, z_up, z_dn, r_halves, "r", r1_left)
        over(k, 0)

    def r2(k):
        gather2(r_ref, k, z_up, z_dn, r_halves, "r", r2_left)

    def rd(k):
        wait(got, f"rrest{k}")
        over(k, 3)
        over(k, 1)

    def re(k):
        wait(got, f"rfar{k}")
        over(k, 2)

    def rf(k):
        wait(got, f"over{k}")

    def c1(b):
        gather1(c_ref, b, y_up, y_dn, c_halves, "c", c1_left)

    def c2(b):
        gather2(c_ref, b, y_up, y_dn, c_halves, "c", c2_left)

    def cf(b):
        wait(got, f"cboth{b}")

    def pick(s, values):
        out = values[0]
        for i in range(1, len(values)):
            out = jnp.where(s == i, values[i], out)
        return out

    def block(s):
        k, j, j2 = (pick(s, [block[i] for block in ORDER]) for i in range(3))
        groups = [(rz, rc, ry) for rz in range(4) for rc in range(2) for ry in range(4)]
        lhs = jnp.concatenate([rbuf[k, rz, rc, ry] for rz, rc, ry in groups], axis=1)
        early = (j == NJ - 1) & (j2 == NJ - 1)
        far, far2 = jnp.where(early, NJ, j), jnp.where(early, NJ, j2)
        left = jnp.concatenate([cbuf[far if ry == 2 else j, ry, rz * 2 + rc] for rz, rc, ry in groups], axis=0)
        right = jnp.concatenate([cbuf[far2 if ry == 2 else j2, ry, rz * 2 + rc] for rz, rc, ry in groups], axis=0)
        value = jnp.dot(lhs, jnp.concatenate([left, right], axis=1), preferred_element_type=F32)
        last = k == NA - 1
        own[jnp.where(last, j, jnp.where(early, NJ + 1 + k, NJ))] = value[:, :TB]
        own[jnp.where(last, j2, NJ)] = value[:, TB:]
        rss[j, k] = value[:, :TB].astype(BF16)
        rss[j2, k] = value[:, TB:].astype(BF16)

        pl.when(jnp.logical_not(early))(lambda: reduce_tile(j, k))
        pl.when(j2 > j)(lambda: reduce_tile(j2, k))

    def late(k, carry):
        lhs = jnp.concatenate([rbuf[k, rz, rc, 2] for rz in range(4) for rc in range(2)], axis=1)
        right = jnp.concatenate([cbuf[NJ - 1, 2, i] for i in range(8)], axis=0)
        value = own[NJ + 1 + k] + jnp.dot(lhs, right, preferred_element_type=F32)
        rss[NJ - 1, k] = value.astype(BF16)
        reduce_tile(NJ - 1, k)
        return carry

    def reduce_tile(j, k):
        @pl.when(k == 0)
        def _():
            reduce(j, k, 0, place(2, 0, 0, 0)).start()

        @pl.when((k == 1) | (k == 2))
        def _():
            reduce(j, k, 1, place(1, 0, 0, 0)).start()
            reduce(j, k, 3, place(3, 0, 0, 0)).start()

    def reduce(j, k, dx, to):
        if dx == 0:
            src, dst = rss.at[j, k], rsr.at[j, 2]
        else:
            src = rss.at[j, k, pl.ds(192 * (dx // 2), 192)]
            dst = rsr.at[j, 4 - dx, pl.ds((k - 1) * 192, 192)]
        return pltpu.make_async_remote_copy(
            src_ref=src, dst_ref=dst, send_sem=sum_ssem, recv_sem=sum_rsem.at[jnp.where(j == NJ - 1, 1, 0)],
            device_id=to, device_id_type=MESH,
        )

    def small1():
        def partial(t, carry):
            part = jnp.dot(half, jnp.concatenate([wn[2 * t], wn[2 * t + 1]], axis=1), preferred_element_type=F32)
            for i in range(2):
                pall[2 * t + i] = part[0:1, i * TB : (i + 1) * TB]
            return carry

        lax.fori_loop(0, 24, partial, 0, unroll=6)
        for dx in range(4):
            for yy in range(4):
                for i in range(3):
                    t = tile_map[(x + dx) % 4 * 12 + yy * 3 + i]
                    psend[dx, yy, i : i + 1] = pall[t]
        o_in, o_out = (("o1", lambda: obs_all.at[r, pl.ds(0, 7)]),) * 2
        for dz, dc in line:
            send(obs_all.at[r, q], obs_all.at[r, q], dev(dz=dz, dc=dc), o_in, o_out)
        pbuf[x] = psend[0]
        p_in, p_out = ("p1", lambda: pbuf.at[pl.ds(0, 3)]), ("p1", lambda: psend.at[pl.ds(1, 3)])
        for d in (1, 2, 3):
            send(psend.at[d], pbuf.at[x], dev(dx=d), p_in, p_out)

    def small2():
        wait(got, "o1")
        wait(got, "p1")
        o_in, o_out = (("o2", lambda: obs_all.at[pl.ds(0, 3)]),) * 2
        for d in (1, 2, 3):
            send(obs_all.at[r], obs_all.at[r], dev(dy=d), o_in, o_out)
        tot[...] = (pbuf[0] + pbuf[1]) + (pbuf[2] + pbuf[3])
        tbuf[y] = tot[y]
        p_in, p_out = ("p2", lambda: tbuf.at[pl.ds(0, 3)]), ("p2", lambda: tot.at[pl.ds(0, 3)])
        for d in (1, 2, 3):
            send(tot.at[y_of[d]], tbuf.at[y], dev(dy=d), p_in, p_out)

    def small3():
        wait(got, "o2")
        wait(got, "p2")
        o_in, o_out = (("o3", lambda: obs_all.at[pl.ds(0, 12)]),) * 2
        for d in (1, 2, 3):
            send(obs_all.at[x_rows], obs_all.at[x_rows], dev(dx=d), o_in, o_out)
        qbuf[q] = (tbuf[0] + tbuf[1]) + (tbuf[2] + tbuf[3])
        p_in, p_out = (("p3", lambda: qbuf.at[pl.ds(0, 7)]),) * 2
        for dz, dc in line:
            send(qbuf.at[q], qbuf.at[q], dev(dz=dz, dc=dc), p_in, p_out)

    def small4():
        wait(got, "o3")
        wait(got, "p3")
        total = qbuf[0]
        for i in range(1, 8):
            total = total + qbuf[i]
        rhs[...] = total
        every = obs_all[...].reshape(16 * 8, 1, TB)
        block_of = lax.broadcasted_iota(jnp.int32, every.shape, 0)
        bal[...] = jnp.sum(jnp.where(block_of == plan[...], every, 0.0), axis=0)

    first_r = [(dy, i) for dy in (1, 2, 3, 0) for i in range(3)]
    for n in range(0, 12, 2):
        pair = first_r[n : n + 2]
        white = slot_pair(*[(x + R_CH[0][0][0]) % 4 * 12 + (y + dy) % 4 * 3 + i for dy, i in pair])
        flipped = white.T.astype(BF16)
        for m, (dy, i) in enumerate(pair):
            tile, rows = flipped[m * TB : (m + 1) * TB], pl.ds(i * TB, TB)
            if dy == 0:
                rbuf[0, 0, 0, 0, rows] = tile
            else:
                rsend[0, dy - 1, rows] = tile
    pl.semaphore_wait(barrier, len(places))
    spread_r(0)
    for dz, dc in line + [(0, 0)]:
        base = ((z + dz) % 4 * 2 + (c + dc) % 2) * 6
        white = slot_pair(base, base + 1).astype(BF16)
        for j in range(2):
            tile = white[:, j * TB : (j + 1) * TB]
            if (dz, dc) == (0, 0):
                cbuf[j, 0, 0] = tile
            else:
                csend[j, dz * 2 + dc - 1] = tile
    spread_c(0)
    lax.fori_loop(0, 24, whiten_pair, 0, unroll=6)
    stage_r(1)
    stage_c(1)
    spread_r(1)
    spread_c(1)
    stage_r(2)
    stage_c(2)
    stage_r(3)
    stage_c(3)
    spread_r(2)
    spread_c(2)
    cbuf[NJ, 2] = jnp.zeros((8, TB, TB), BF16)
    r1(0)
    c1(0)
    small1()
    r2(0)
    r1(1)
    c2(0)
    c1(1)
    rd(0)
    re(0)
    r2(1)
    r1(2)
    spread_c(3)
    spread_r(3)
    small2()
    rf(0)
    cf(0)
    c2(1)

    def before1():
        rd(1)
        re(1)
        c1(2)
        r2(2)
        r1(3)
        rf(1)

    def before2():
        cf(1)

    def before4():
        c2(2)
        c1(3)
        rd(2)
        re(2)
        rf(2)

    def before6():
        r2(3)
        cf(2)

    def before8():
        c2(3)
        rd(3)

    def before9():
        small3()
        wait(got, "crest3")

    def before11():
        re(3)

    def before12():
        wait(got, "cfar3")
        lax.fori_loop(0, 3, late, 0)
        rf(3)

    acts = (
        (1, before1), (2, before2), (4, before4), (6, before6), (8, before8), (9, before9), (11, before11), (12, before12),
    )

    def slot(s, carry):
        for i, act in acts:
            pl.when(s == i)(act)
        block(s)
        return carry

    lax.fori_loop(0, len(ORDER), slot, 0)
    small4()
    for j in range(NJ):
        if j == 0 or j == NJ - 1:
            arrived = rsr.at[pl.ds(0, NJ - 1) if j == 0 else NJ - 1, pl.ds(1, 3)]
            pltpu.make_async_copy(arrived, arrived, sum_rsem.at[j // (NJ - 1)]).wait()
        total = own[j]
        for dx in (1, 2, 3):
            total = total + rsr[j, dx].astype(F32)
        gram[:, j * TB : (j + 1) * TB] = total
    for name in left:
        wait(left, name)
    sent = rss.at[:, pl.ds(0, 3)]
    pltpu.make_async_copy(sent, sent, sum_ssem).wait()


def hand_over(gram, rhs, bal, gram_out, rhs_out, bal_out, flat, sem):
    for i in range(3):
        flat[i * TB : (i + 1) * TB] = rhs[i]
    rows = [pl.ds(i * 96, 96) for i in range(4)]
    pairs = [(gram.at[part], gram_out.at[part]) for part in rows] + [(bal, bal_out), (flat, rhs_out)]
    copies = [pltpu.make_async_copy(src, dst, sem.at[i]) for i, (src, dst) in enumerate(pairs)]
    for cp in copies:
        cp.start()
    for cp in copies:
        cp.wait()


def on_device(
    design, observations, gaps, noise_var, arc_lengths, arc_amp, arc_decay, plan, tile_map
):
    vmem = pl.BlockSpec(memory_space=pltpu.VMEM)
    gram, rhs, bal = pl.pallas_call(
        kernel,
        name="normal_equations",
        out_shape=(
            pltpu.VMEM((384, 768), F32),
            pltpu.VMEM((3, TB), F32),
            pltpu.VMEM((1, TB), F32),
        ),
        in_specs=[pl.BlockSpec(memory_space=pl.ANY)] * 9,
        out_specs=(vmem, vmem, vmem),
        scratch_shapes=[
            pltpu.SMEM((48,), jnp.int32),
            pltpu.SMEM((1, 4), jnp.int32),
            pltpu.SMEM((1, 4), F32),
            pltpu.SMEM((1, 4), F32),
            pltpu.VMEM((1, 1), jnp.int32),
            pltpu.VMEM((1, TB), F32),
            pltpu.VMEM((1, TB), jnp.int32),
            pltpu.VMEM((1, TB), F32),
            pltpu.VMEM((48, TB, TB), BF16),
            pltpu.VMEM((48, TB, TB), BF16),
            pltpu.VMEM((48, TB, TB), BF16),
            pltpu.VMEM((48, 1, TB), F32),
            pltpu.VMEM((NA, 4, 2, 4, 384, TB), BF16),
            pltpu.VMEM((NA, 3, 384, TB), BF16),
            pltpu.VMEM((NJ + 1, 4, 8, TB, TB), BF16),
            pltpu.VMEM((NJ, 7, TB, TB), BF16),
            pltpu.VMEM((NJ + 4, 384, TB), F32),
            pltpu.VMEM((NJ, 4, 384, TB), BF16),
            pltpu.VMEM((NJ, 4, 384, TB), BF16),
            pltpu.VMEM((16, 8, 1, TB), F32),
            pltpu.VMEM((4, 4, 3, TB), F32),
            pltpu.VMEM((4, 4, 3, TB), F32),
            pltpu.VMEM((8, 3, TB), F32),
            pltpu.VMEM((4, 3, TB), F32),
            pltpu.VMEM((4, 3, TB), F32),
            pltpu.SemaphoreType.DMA((8,)),
            pltpu.SemaphoreType.DMA,
            pltpu.SemaphoreType.DMA((N_LEFT,)),
            pltpu.SemaphoreType.DMA((N_GOT,)),
            pltpu.SemaphoreType.DMA,
            pltpu.SemaphoreType.DMA((2,)),
        ],
        compiler_params=pltpu.CompilerParams(
            collective_id=0, has_side_effects=True, vmem_limit_bytes=60 * 1024 * 1024
        ),
    )(
        tile_map,
        arc_lengths,
        arc_amp,
        arc_decay,
        plan.reshape(1, 1),
        design,
        observations.reshape(1, TB),
        gaps.reshape(1, TB),
        noise_var.reshape(1, TB),
    )
    inner = [pltpu.with_memory_space_constraint(v, pltpu.VMEM) for v in (gram, rhs, bal)]
    anywhere = pl.BlockSpec(memory_space=pl.ANY)
    return pl.pallas_call(
        hand_over,
        name="hand_over",
        out_shape=(
            jax.ShapeDtypeStruct((384, 768), F32),
            jax.ShapeDtypeStruct((384,), F32),
            jax.ShapeDtypeStruct((1, TB), F32),
        ),
        in_specs=[vmem] * 3,
        out_specs=(anywhere, anywhere, anywhere),
        scratch_shapes=[pltpu.VMEM((384,), F32), pltpu.SemaphoreType.DMA((6,))],
        compiler_params=pltpu.CompilerParams(vmem_limit_bytes=1024 * 1024),
    )(*inner)


def solution(mesh):
    placed = (
        P(("row", "col"), None),
        P(("row", "col")),
        P(("row", "col")),
        P(("row", "col")),
        P(("row", "col"), None),
        P(("row", "col"), None),
        P(("row", "col"), None),
        P(("row", "col")),
        P(),
    )
    return jax.shard_map(
        on_device,
        mesh=mesh,
        in_specs=placed,
        out_specs=(P("row", "col"), P("row"), P(("row", "col"), None)),
        check_vma=False,
    )
```
